256 devices in a mesh: band: 64 (over x, z_lo, y, core), pw: 4 (over z_hi).
Axes of the slice: x: 4, y: 4, z: 8 (z_hi: 4, z_lo: 2; z = z_hi * 2 + z_lo), core: 2. Of those that a mesh axis runs over, the one named last changes fastest.
Arguments:
- pair_density: bfloat16 [320, 128, 9216], P('band', None, 'pw'), may hold values from -6 to 6
- eigvecs: bfloat16 [2944, 9216], P('band', 'pw'), may hold values from -0.0625 to 0.0625
- screening: bfloat16 [2944, 2944], P('pw'), may hold values from -0.00048828125 to 0.00048828125
- occupation: float32 [128], replicated, may hold values from 0 to 1
- window_start: int32 [320], P('band'), may hold values from 0 to 511, as said below
- window_len: int32 [320], P('band'), may hold values from 1 to 128, as said below
- slot_band: int32 [320], P('band'), may hold values from -1 to 127, as said below
Outputs:
- sigma: float32 [512, 512], P(('band', 'pw'))
The draws below stay inside these ranges and needn't reach their ends.
Inputs may be any that keep to these rules, and one draw needn't show every extreme that they name: window_start + window_len <= 512 for every slot. `window_len`: some slot has a window of 128 bands. On each index of band the live slots (slot_band >= 0) come first among its 5 slots; each index holds 3 to 5 live slots, and the counts of index i and index i + 64 / 2 add up to 8.
All inputs are finite; a program needn't handle non-finite values.
Results may differ from the reference program's by a relative error of at most 0.0049.
Values may be sent and summed in bfloat16 or wider, within the bound.
A program may use at most 128 MiB of HBM per device.

```python
import jax
import jax.numpy as jnp
from jax import lax

NB_SIGMA = 512
BLOCK = 128
G = 9216
S = 2944
CAP = 5
SLOTS = 320
NSUM = 128


def window_parts(key):
    lengths = jax.random.randint(jax.random.fold_in(key, 11), (SLOTS,), 1, BLOCK + 1)
    lengths = lengths.at[0].set(BLOCK)
    lengths = lengths.at[1].set(1)
    spaces = NB_SIGMA - lengths + 1
    raw_bits = jax.random.randint(jax.random.fold_in(key, 12), (SLOTS,), 0, 1 << 30)
    starts = raw_bits % spaces
    starts = starts.at[0].set(0)
    starts = starts.at[1].set(NB_SIGMA - 1)
    return (starts.astype(jnp.int32), lengths.astype(jnp.int32))


def draw_window_start(key, part):
    starts, lengths = window_parts(key)
    return starts


def draw_window_len(key, part):
    starts, lengths = window_parts(key)
    return lengths


def draw_slot_band(key, part):
    groups = SLOTS // CAP
    halves = groups // 2
    lower = jax.random.randint(jax.random.fold_in(key, 21), (halves,), CAP - 2, CAP + 1)
    counts = jnp.concatenate([lower, 2 * CAP - 2 - lower])
    position = jnp.arange(SLOTS, dtype=jnp.int32) % CAP
    device = jnp.arange(SLOTS, dtype=jnp.int32) // CAP
    band_ids = jax.random.randint(jax.random.fold_in(key, 22), (SLOTS,), 0, NSUM)
    return jnp.where(position < counts[device], band_ids, -1).astype(jnp.int32)


def steps_of(own_key, extent, pieces, least, top_value):
    def one(axis_at, parts):
        heights = jax.random.uniform(jax.random.fold_in(jax.random.fold_in(own_key, 6), axis_at), (parts,), jnp.float32, least / len(pieces), top_value / len(pieces))
        return jnp.repeat(jnp.exp(heights), extent[axis_at] // parts).reshape((-1,) + (1,) * (len(extent) - axis_at - 1))

    level = one(*pieces[0])
    for cut in pieces[1:]:
        level = level * one(*cut)
    return level


def noise(own_key, shape, width, bound, pieces=(), kind=jnp.bfloat16):
    result = jax.random.normal(own_key, shape, jnp.float32) * width
    if len(pieces) > 0:
        result = steps_of(own_key, shape, pieces, -0.22, 0.18) * result
    return jnp.clip(result, min=-bound, max=bound).astype(kind)


def setup_inputs(seed: int = 0) -> dict:
    streams_of = jax.random.split(jax.random.key(seed), 8)
    return {
        "pair_density": noise(streams_of[0], (SLOTS, BLOCK, G), 1.0, 6.0, ((0, 64), (2, 4))),
        "eigvecs": noise(streams_of[1], (S, G), G ** -0.5, 0.0625, ((0, 64), (1, 4))),
        "screening": noise(streams_of[2], (S, S), (16 * S * S) ** -0.5, 0.00048828125, ((0, 4),)),
        "occupation": jnp.clip(jax.random.uniform(streams_of[3], (NSUM,), jnp.float32, 0.0, 1.0), 0.0, 1.0),
        "window_start": draw_window_start(jax.random.fold_in(streams_of[7], 71), 0),
        "window_len": draw_window_len(jax.random.fold_in(streams_of[7], 71), 0),
        "slot_band": draw_slot_band(jax.random.fold_in(streams_of[7], 71), 0),
    }


def reference(pair_density, eigvecs, screening, occupation, window_start, window_len, slot_band):
    row_ids = jnp.arange(BLOCK, dtype=jnp.int32)
    band_list = jnp.arange(NSUM, dtype=jnp.int32)

    def add_slot(totals, item):
        density, offset, length, band_id = item
        raw_proj = jnp.dot(density, eigvecs.T, preferred_element_type=jnp.float32)
        keep_rows = ((row_ids < length) & (band_id >= 0)).astype(jnp.float32)
        projected = (raw_proj * keep_rows[:, None]).astype(jnp.bfloat16)
        screened = jnp.dot(projected, screening.T, preferred_element_type=jnp.float32).astype(jnp.bfloat16)
        block_sigma = jnp.dot(screened, projected.T, preferred_element_type=jnp.float32)
        weight = 0.5 - jnp.sum(jnp.where(band_list == band_id, occupation, jnp.zeros_like(occupation)))
        first = offset.astype(jnp.int32)
        previous = lax.dynamic_slice(totals, (first, first), (BLOCK, BLOCK))
        totals = lax.dynamic_update_slice(totals, previous + weight * block_sigma, (first, first))
        return totals, None

    start_sum = jnp.zeros((NB_SIGMA + BLOCK, NB_SIGMA + BLOCK), jnp.float32)
    totals, unused = lax.scan(add_slot, start_sum, (pair_density, window_start, window_len, slot_band))
    return totals[:NB_SIGMA, :NB_SIGMA]
```

```python
import jax
import jax.numpy as jnp
from jax import lax
from jax.experimental import pallas as pl
from jax.experimental.pallas import tpu as pltpu
from jax.sharding import PartitionSpec as P

NB_SIGMA = 512
BLOCK = 128
F32 = jnp.float32
BF16 = jnp.bfloat16
SHARE, PADDED = 46, 48
CHUNK = 8 * PADDED
WROWS, WCOLS = 96, 768

N_COPIES = 160


def main_kernel(
    taking_ref,
    meta_ref,
    a_ref,
    eig_ref,
    w_ref,
    bs_ref,
    meta_out,
    a_all,
    spare,
    own3,
    bbuf,
    wbuf,
    part,
    hop_s,
    hop_r,
    dir_s,
    dir_r,
    comb_s,
    comb_r,
    pt,
    ptd,
    pth,
    scr,
    meta_buf,
    ssem,
    rsem,
    lsem,
):
    band = lax.axis_index("band")
    h = lax.axis_index("pw")
    x = band // 16
    zl = (band // 8) % 2
    y = (band // 2) % 4
    c = band % 2
    u = x * (1 - c) + y * c
    v = y * (1 - c) + x * c
    su = 16 - 14 * c
    sv = 2 + 14 * c
    hp, hm, h2 = (h + 1) % 4, (h + 3) % 4, (h + 2) % 4
    up, um, u2 = (u + 1) % 4, (u + 3) % 4, (u + 2) % 4
    vp, vm, v2 = (v + 1) % 4, (v + 3) % 4, (v + 2) % 4

    def at_uv(uu, vv):
        return (uu * su + vv * sv + zl * 8 + c, h)

    dev_up, dev_um = at_uv(up, v), at_uv(um, v)
    dev_vp, dev_vm = at_uv(u, vp), at_uv(u, vm)
    dev_hp, dev_hm = (band, hp), (band, hm)
    dev_zl = (x * 16 + (1 - zl) * 8 + y * 2 + c, h)
    dev_mate = (x * 16 + zl * 8 + y * 2 + 1 - c, h)
    dev_far = (((x + 2) % 4) * 16 + zl * 8 + y * 2 + c, h)

    barrier = pltpu.get_barrier_semaphore()
    peers = [dev_up, dev_um, dev_vp, dev_vm, dev_hp, dev_hm, dev_zl, dev_mate, dev_far]
    for peer in peers:
        pl.semaphore_signal(barrier, inc=1, device_id=peer, device_id_type=pl.DeviceIdType.MESH)
    pl.semaphore_wait(barrier, len(peers))

    ids = {}
    sent = []

    def remote(name, src, dst, device):
        i = ids.setdefault(name, len(ids))
        return pltpu.make_async_remote_copy(
            src_ref=src,
            dst_ref=dst,
            send_sem=ssem.at[i],
            recv_sem=rsem.at[i],
            device_id=device,
            device_id_type=pl.DeviceIdType.MESH,
        )

    def send(name, src, dst, device):
        copy = remote(name, src, dst, device)
        copy.start()
        sent.append(copy)

    def got(name, landing, device):
        remote(name, landing, landing, device).wait_recv()

    local_ids = {}

    def local(name, src, dst):
        i = local_ids.setdefault(name, len(local_ids))
        return pltpu.make_async_copy(src, dst, lsem.at[i])

    send("zl", eig_ref, bbuf.at[v, u, zl], dev_zl)
    own_b = local("b", eig_ref, bbuf.at[v, u, zl])
    own_b.start()
    send("spare", a_ref.at[4], spare, dev_far)
    send("meta_far", meta_ref, meta_buf.at[1], dev_far)
    send("meta_mate", meta_ref, meta_buf.at[2], dev_mate)
    own_a = []
    for j in range(3):
        own_a.append(local(f"a{j}", a_ref.at[j], a_all.at[2 * j + c]))
        own_a[-1].start()
        send(f"mate_a{j}", a_ref.at[j], a_all.at[2 * j + c], dev_mate)
    own_a.append(local("a3", a_ref.at[3], own3))
    own_a[-1].start()

    def w_slice(p, q):
        row = pl.multiple_of(c * 368 + p * WROWS - 16 * (p // 3), 16)
        col = pl.multiple_of(q * WCOLS - 128 * (q // 3), 128)
        return w_ref.at[pl.ds(row, WROWS), pl.ds(col, WCOLS)]

    send("wz_m", w_slice(u, v), wbuf.at[1, u, v], dev_hm)
    send("wz_p", w_slice(u, v), wbuf.at[3, u, v], dev_hp)
    own_w = []
    for p in range(4):
        for q in range(4):
            own_w.append(local(f"w{p}{q}", w_slice(p, q), wbuf.at[0, p, q]))
            own_w[-1].start()

    own_b.wait()
    got("zl", bbuf.at[v, u, 1 - zl], dev_zl)

    def v_send(kind, buf_at, uu, tag):
        send(f"{kind}v_p{tag}", buf_at(uu, v), buf_at(uu, v), dev_vp)
        send(f"{kind}v_m{tag}", buf_at(uu, v), buf_at(uu, v), dev_vm)

    def b_at(uu, vv):
        return bbuf.at[vv, uu]

    def w_at(uu, vv):
        return wbuf.at[pl.ds(1, 3), uu, vv]

    send("bu_p", b_at(u, v), b_at(u, v), dev_up)
    send("bu_m", b_at(u, v), b_at(u, v), dev_um)
    v_send("b", b_at, u, 0)
    got("bu_p", b_at(um, v), dev_um)
    send("buf_p", bbuf.at[v, um, 0], bbuf.at[v, um, 0], dev_up)
    v_send("b", b_at, um, 1)
    got("bu_m", b_at(up, v), dev_up)
    send("buf_m", bbuf.at[v, up, 1], bbuf.at[v, up, 1], dev_um)
    v_send("b", b_at, up, 2)

    lower, upper = pl.ds(0, WROWS // 2), pl.ds(WROWS // 2, WROWS // 2)
    got("wz_m", wbuf.at[1, u, v], dev_hp)
    send("wzf_m", wbuf.at[1, u, v, lower], wbuf.at[2, u, v, lower], dev_hm)
    got("wz_p", wbuf.at[3, u, v], dev_hm)
    send("wzf_p", wbuf.at[3, u, v, upper], wbuf.at[2, u, v, upper], dev_hp)

    got("buf_p", bbuf.at[v, u2, 0], dev_um)
    got("buf_m", bbuf.at[v, u2, 1], dev_up)
    v_send("b", b_at, u2, 3)

    got("meta_far", meta_buf.at[1], dev_far)
    send("meta_mate_far", meta_buf.at[1], meta_buf.at[3], dev_mate)
    got("spare", spare, dev_far)
    own_a[3].wait()
    taking = taking_ref[0] == 1
    a_all[6 + c] = jnp.where(taking, spare[...], own3[...])
    send("mate_a3", a_all.at[6 + c], a_all.at[6 + c], dev_mate)

    got("wzf_m", wbuf.at[2, u, v, lower], dev_hp)
    got("wzf_p", wbuf.at[2, u, v, upper], dev_hm)
    send("wu_p", w_at(u, v), w_at(u, v), dev_up)
    send("wu_m", w_at(u, v), w_at(u, v), dev_um)

    for j in range(3):
        own_a[j].wait()
        got(f"mate_a{j}", a_all.at[2 * j + 1 - c], dev_mate)
    got("mate_a3", a_all.at[7 - c], dev_mate)

    left, right = pl.ds(0, BLOCK), pl.ds(BLOCK, BLOCK)

    def compute(k, vk):
        @pl.loop(0, 4)
        def _(d):
            part[k, d] = lax.dot_general(
                bbuf[vk].reshape(CHUNK, bbuf.shape[-1]),
                a_all[pl.ds(2 * d, 2)].reshape(2 * BLOCK, bbuf.shape[-1]),
                (((1,), (1,)), ((), ())),
                preferred_element_type=F32,
            )

        hop_s[k, 0] = part[k, h2, :, left].astype(BF16)
        send(f"hop{k}0", hop_s.at[k, 0], hop_r.at[k, 0], dev_hm)
        hop_s[k, 1] = part[k, h2, :, right].astype(BF16)
        send(f"hop{k}1", hop_s.at[k, 1], hop_r.at[k, 1], dev_hp)
        dir_s[k, 0] = part[k, hm, :, right].astype(BF16)
        send(f"dir{k}0", dir_s.at[k, 0], dir_r.at[k, 0], dev_hm)
        dir_s[k, 1] = part[k, hp, :, left].astype(BF16)
        send(f"dir{k}1", dir_s.at[k, 1], dir_r.at[k, 1], dev_hp)

    def combine(k):
        got(f"hop{k}0", hop_r.at[k, 0], dev_hp)
        comb_s[k, 0] = (part[k, hm, :, left] + hop_r[k, 0].astype(F32)).astype(BF16)
        send(f"comb{k}0", comb_s.at[k, 0], comb_r.at[k, 0], dev_hm)
        got(f"hop{k}1", hop_r.at[k, 1], dev_hm)
        comb_s[k, 1] = (part[k, hp, :, right] + hop_r[k, 1].astype(F32)).astype(BF16)
        send(f"comb{k}1", comb_s.at[k, 1], comb_r.at[k, 1], dev_hp)

    def finish(k, vk):
        got(f"dir{k}0", dir_r.at[k, 0], dev_hp)
        got(f"dir{k}1", dir_r.at[k, 1], dev_hm)
        got(f"comb{k}0", comb_r.at[k, 0], dev_hp)
        got(f"comb{k}1", comb_r.at[k, 1], dev_hm)
        pt[c, vk, :, left] = part[k, h, :, left] + (
            comb_r[k, 0].astype(F32) + dir_r[k, 1].astype(F32)
        )
        pt[c, vk, :, right] = part[k, h, :, right] + (
            comb_r[k, 1].astype(F32) + dir_r[k, 0].astype(F32)
        )
        send(f"pt{k}", pt.at[c, vk], pt.at[c, vk], dev_mate)

    compute(0, v)

    around = (u, um, up, u2)
    for tag in range(4):
        got(f"bv_p{tag}", b_at(around[tag], vm), dev_vm)
        if tag < 2:
            send(f"bvf_p{tag}", b_at(around[tag], vm), b_at(around[tag], vm), dev_vp)
    for tag in range(4):
        got(f"bv_m{tag}", b_at(around[tag], vp), dev_vp)
        if tag >= 2:
            send(f"bvf_m{tag}", b_at(around[tag], vp), b_at(around[tag], vp), dev_vm)

    v_send("w", w_at, u, 0)
    three = pl.ds(1, 3)
    got("wu_p", w_at(um, v), dev_um)
    send("wuf_p", wbuf.at[three, um, v, lower], wbuf.at[three, um, v, lower], dev_up)
    v_send("w", w_at, um, 1)
    got("wu_m", w_at(up, v), dev_up)
    send("wuf_m", wbuf.at[three, up, v, upper], wbuf.at[three, up, v, upper], dev_um)
    v_send("w", w_at, up, 2)

    compute(1, vm)
    combine(0)
    compute(2, vp)
    combine(1)
    finish(0, v)

    got("wuf_p", wbuf.at[three, u2, v, lower], dev_um)
    got("wuf_m", wbuf.at[three, u2, v, upper], dev_up)
    v_send("w", w_at, u2, 3)

    for tag in range(4):
        if tag < 2:
            got(f"bvf_p{tag}", b_at(around[tag], v2), dev_vm)
        else:
            got(f"bvf_m{tag}", b_at(around[tag], v2), dev_vp)
    compute(3, v2)
    combine(2)
    finish(1, vm)
    combine(3)

    for tag in range(4):
        got(f"wv_p{tag}", w_at(around[tag], vm), dev_vm)
        if tag < 2:
            send(f"wvf_p{tag}", w_at(around[tag], vm), w_at(around[tag], vm), dev_vp)
    for tag in range(4):
        got(f"wv_m{tag}", w_at(around[tag], vp), dev_vp)
        if tag >= 2:
            send(f"wvf_m{tag}", w_at(around[tag], vp), w_at(around[tag], vp), dev_vm)

    finish(2, vp)
    finish(3, v2)
    order = (v, vm, vp, v2)
    for k in range(4):
        got(f"pt{k}", pt.at[1 - c, order[k]], dev_mate)

    for src in range(2):
        for vv in range(4):
            for uu in range(4):
                for zz in range(2):
                    xx, yy = (uu, vv) if src == 0 else (vv, uu)
                    first = SHARE * (xx * 16 + zz * 8 + yy * 2 + src)
                    row = PADDED * (2 * uu + zz)
                    ptd[first : first + SHARE, :] = pt[src, vv, row : row + SHARE, :]
    pth[...] = ptd[...].astype(BF16)

    for copy in own_w:
        copy.wait()
    for tag in range(4):
        if tag < 2:
            got(f"wvf_p{tag}", w_at(around[tag], v2), dev_vm)
        else:
            got(f"wvf_m{tag}", w_at(around[tag], v2), dev_vp)

    for q in range(4):
        skip = 128 if q == 3 else 0

        @pl.loop(0, 4)
        def _(rel):
            value = jnp.dot(
                wbuf[rel, :, q, :, skip:].reshape(4 * WROWS, WCOLS - skip),
                pth[WCOLS * q : WCOLS * (q + 1) - skip, :],
                preferred_element_type=F32,
            )
            if q == 0:
                scr[rel] = value
            else:
                scr[rel] += value

    for slot in range(2):
        lanes = pl.ds(slot * BLOCK, BLOCK)
        total = jnp.zeros((BLOCK, BLOCK), F32)
        for rel in range(4):
            base = ((h + rel) % 4) * 736 + c * 368
            for skip, first, count in ((0, 0, 288), (304, 288, 80)):
                rows = pl.ds(pl.multiple_of(base + first, 16), count)
                total += lax.dot_general(
                    scr[rel, pl.ds(skip, count), lanes],
                    ptd[rows, lanes],
                    (((0,), (0,)), ((), ())),
                    preferred_element_type=F32,
                    precision=lax.Precision.HIGHEST,
                )
        bs_ref[slot] = total

    got("meta_mate", meta_buf.at[2], dev_mate)
    got("meta_mate_far", meta_buf.at[3], dev_mate)
    meta_out[0] = meta_ref[...]
    for i in range(1, 4):
        meta_out[i] = meta_buf[i]
    for copy in sent:
        copy.wait_send()
    assert len(ids) <= N_COPIES


def summed_on_arrival(array, axis, dim):
    length = lax.axis_size(axis)
    lengths = array.shape
    blocks = array.reshape(*lengths[:dim], length, lengths[dim] // length, *lengths[dim + 1 :])
    blocks = jnp.moveaxis(blocks, dim, 0)
    arrived = lax.all_to_all(blocks, axis, split_axis=0, concat_axis=0, tiled=True)
    return arrived.astype(F32).sum(axis=0)


def per_device(pair_density, eigvecs, screening, occupation, window_start, window_len, slot_band):
    capacity, block, plane_rows = pair_density.shape
    live_count = jnp.sum((slot_band >= 0).astype(jnp.int32))
    taking = (live_count == capacity - 2).astype(jnp.int32).reshape(1)
    meta = jnp.pad(
        jnp.stack([window_start, window_len, slot_band]), ((0, 5), (0, 128 - capacity))
    )
    eig = jnp.pad(eigvecs, ((0, PADDED - SHARE), (0, 0)))
    width = screening.shape[1]
    vmem = pl.BlockSpec(memory_space=pltpu.VMEM)
    hbm = pl.BlockSpec(memory_space=pltpu.HBM)
    scratch = [
        pltpu.VMEM((8, block, plane_rows), BF16),
        pltpu.VMEM((block, plane_rows), BF16),
        pltpu.VMEM((block, plane_rows), BF16),
        pltpu.VMEM((4, 4, 2, PADDED, plane_rows), BF16),
        pltpu.VMEM((4, 4, 4, WROWS, WCOLS), BF16),
        pltpu.VMEM((4, 4, CHUNK, 2 * block), F32),
    ]
    scratch += [pltpu.VMEM((4, 2, CHUNK, block), BF16)] * 6
    scratch += [
        pltpu.VMEM((2, 4, CHUNK, 2 * block), F32),
        pltpu.VMEM((width, 2 * block), F32),
        pltpu.VMEM((width, 2 * block), BF16),
        pltpu.VMEM((4, 4 * WROWS, 2 * block), F32),
        pltpu.VMEM((4, 8, 128), jnp.int32),
        pltpu.SemaphoreType.DMA((N_COPIES,)),
        pltpu.SemaphoreType.DMA((N_COPIES,)),
        pltpu.SemaphoreType.DMA((24,)),
    ]
    block_sigma, metas = pl.pallas_call(
        main_kernel,
        out_shape=(
            jax.ShapeDtypeStruct((2, block, block), F32),
            jax.ShapeDtypeStruct((4, 8, 128), jnp.int32),
        ),
        in_specs=[pl.BlockSpec(memory_space=pltpu.SMEM), vmem, hbm, hbm, hbm],
        out_specs=(vmem, vmem),
        scratch_shapes=scratch,
        compiler_params=pltpu.CompilerParams(
            collective_id=0, has_side_effects=True, vmem_limit_bytes=60 * 1024 * 1024
        ),
        name="project_and_screen",
    )(taking, meta, pair_density, eig, screening)

    core = lax.axis_index("band") % 2
    index = lax.axis_index("pw")
    last = capacity - 1
    totals = jnp.zeros((NB_SIGMA + block, NB_SIGMA + block), F32)
    row_ids = jnp.arange(block, dtype=jnp.int32)
    band_list = jnp.arange(occupation.shape[0], dtype=jnp.int32)
    for slot in range(2):
        is_own = core == slot
        own = jnp.where(is_own, metas[0], metas[2])
        far = jnp.where(is_own, metas[1], metas[3])
        count = jnp.sum((own[2, :capacity] >= 0).astype(jnp.int32))
        swap = (count == capacity - 2) & (index == last - 1)
        mine = lax.dynamic_slice(own, (0, index), (8, 1))[:, 0]
        chosen = jnp.where(swap, far[:, last], mine)
        first, length, band_id = chosen[0], chosen[1], chosen[2]
        keep = ((row_ids < length) & (band_id >= 0)).astype(F32)
        weight = 0.5 - jnp.sum(jnp.where(band_list == band_id, occupation, 0.0))
        piece = block_sigma[slot] * (weight * keep[:, None] * keep[None, :])
        previous = lax.dynamic_slice(totals, (first, first), (block, block))
        totals = lax.dynamic_update_slice(totals, previous + piece, (first, first))
    sigma_part = totals[:NB_SIGMA, :NB_SIGMA]
    by_band = summed_on_arrival(sigma_part.astype(BF16), "band", 0)
    return summed_on_arrival(by_band, "pw", 0)


def solution(mesh):
    return jax.shard_map(
        per_device,
        mesh=mesh,
        in_specs=(
            P("band", None, "pw"),
            P("band", "pw"),
            P("pw", None),
            P(),
            P("band"),
            P("band"),
            P("band"),
        ),
        out_specs=P(("band", "pw"), None),
        check_vma=False,
    )
```

```python
import jax
import jax.numpy as jnp
from jax import lax
from jax.experimental import pallas as pl
from jax.experimental.pallas import tpu as pltpu
from jax.sharding import PartitionSpec as P

NB_SIGMA = 512
BLOCK = 128
F32 = jnp.float32
BF16 = jnp.bfloat16
SHARE, PADDED = 46, 48
CHUNK = 8 * PADDED
WROWS, WCOLS = 96, 768

N_COPIES = 160


def main_kernel(
    start_ref,
    len_ref,
    slot_ref,
    occ_ref,
    a_ref,
    eig_ref,
    w_ref,
    out_ref,
    a_all,
    spare,
    own3,
    bbuf,
    wbuf,
    part,
    hop_s,
    hop_r,
    dir_s,
    dir_r,
    comb_s,
    comb_r,
    pt,
    ptd,
    pth,
    scr,
    meta_buf,
    bs_own,
    bs_mate,
    plane_s,
    plane_r,
    line_s,
    line_r,
    ssem,
    rsem,
    lsem,
):
    band = lax.axis_index("band")
    h = lax.axis_index("pw")
    x = band // 16
    zl = (band // 8) % 2
    y = (band // 2) % 4
    c = band % 2
    u = x * (1 - c) + y * c
    v = y * (1 - c) + x * c
    su = 16 - 14 * c
    sv = 2 + 14 * c
    hp, hm, h2 = (h + 1) % 4, (h + 3) % 4, (h + 2) % 4
    up, um, u2 = (u + 1) % 4, (u + 3) % 4, (u + 2) % 4
    vp, vm, v2 = (v + 1) % 4, (v + 3) % 4, (v + 2) % 4

    def at_uv(uu, vv):
        return (uu * su + vv * sv + zl * 8 + c, h)

    dev_up, dev_um = at_uv(up, v), at_uv(um, v)
    dev_vp, dev_vm = at_uv(u, vp), at_uv(u, vm)
    dev_hp, dev_hm = (band, hp), (band, hm)
    dev_zl = (x * 16 + (1 - zl) * 8 + y * 2 + c, h)
    dev_mate = (x * 16 + zl * 8 + y * 2 + 1 - c, h)
    dev_far = (((x + 2) % 4) * 16 + zl * 8 + y * 2 + c, h)

    barrier = pltpu.get_barrier_semaphore()
    plane = {}
    for dx in range(4):
        for dy in range(4):
            if dx or dy:
                place = ((x + dx) % 4, (y + dy) % 4)
                plane[dx, dy] = place, (place[0] * 16 + zl * 8 + place[1] * 2 + c, h)
    line = {}
    for dz in range(2):
        for dh in range(4):
            if dz or dh:
                place = ((zl + dz) % 2, (h + dh) % 4)
                line[dz, dh] = place, (x * 16 + place[0] * 8 + y * 2 + c, place[1])
    peers = [dev_mate] + [device for _, device in [*plane.values(), *line.values()]]
    for peer in peers:
        pl.semaphore_signal(barrier, inc=1, device_id=peer, device_id_type=pl.DeviceIdType.MESH)
    pl.semaphore_wait(barrier, len(peers))

    ids = {}
    sent = []

    def remote(name, src, dst, device):
        i = ids.setdefault(name, len(ids))
        return pltpu.make_async_remote_copy(
            src_ref=src,
            dst_ref=dst,
            send_sem=ssem.at[i],
            recv_sem=rsem.at[i],
            device_id=device,
            device_id_type=pl.DeviceIdType.MESH,
        )

    def send(name, src, dst, device):
        copy = remote(name, src, dst, device)
        copy.start()
        sent.append(copy)

    def got(name, landing, device):
        remote(name, landing, landing, device).wait_recv()

    local_ids = {}

    def local(name, src, dst):
        i = local_ids.setdefault(name, len(local_ids))
        return pltpu.make_async_copy(src, dst, lsem.at[i])

    send("zl", eig_ref, bbuf.at[v, u, zl], dev_zl)
    own_b = local("b", eig_ref, bbuf.at[v, u, zl])
    own_b.start()
    send("spare", a_ref.at[4], spare, dev_far)
    own_a = []
    for j in range(3):
        own_a.append(local(f"a{j}", a_ref.at[j], a_all.at[2 * j + c]))
        own_a[-1].start()
        send(f"mate_a{j}", a_ref.at[j], a_all.at[2 * j + c], dev_mate)
    own_a.append(local("a3", a_ref.at[3], own3))
    own_a[-1].start()

    def w_slice(p, q):
        row = pl.multiple_of(c * 368 + p * WROWS - 16 * (p // 3), 16)
        col = pl.multiple_of(q * WCOLS - 128 * (q // 3), 128)
        return w_ref.at[pl.ds(row, WROWS), pl.ds(col, WCOLS)]

    send("wz_m", w_slice(u, v), wbuf.at[1, u, v], dev_hm)
    send("wz_p", w_slice(u, v), wbuf.at[3, u, v], dev_hp)
    own_w = []
    for p in range(4):
        for q in range(4):
            own_w.append(local(f"w{p}{q}", w_slice(p, q), wbuf.at[0, p, q]))
            own_w[-1].start()

    own_b.wait()
    got("zl", bbuf.at[v, u, 1 - zl], dev_zl)

    def v_send(kind, buf_at, uu, tag):
        send(f"{kind}v_p{tag}", buf_at(uu, v), buf_at(uu, v), dev_vp)
        send(f"{kind}v_m{tag}", buf_at(uu, v), buf_at(uu, v), dev_vm)

    def b_at(uu, vv):
        return bbuf.at[vv, uu]

    def w_at(uu, vv):
        return wbuf.at[pl.ds(1, 3), uu, vv]

    send("bu_p", b_at(u, v), b_at(u, v), dev_up)
    send("bu_m", b_at(u, v), b_at(u, v), dev_um)
    v_send("b", b_at, u, 0)
    got("bu_p", b_at(um, v), dev_um)
    send("buf_p", bbuf.at[v, um, 0], bbuf.at[v, um, 0], dev_up)
    v_send("b", b_at, um, 1)
    got("bu_m", b_at(up, v), dev_up)
    send("buf_m", bbuf.at[v, up, 1], bbuf.at[v, up, 1], dev_um)
    v_send("b", b_at, up, 2)

    lower, upper = pl.ds(0, WROWS // 2), pl.ds(WROWS // 2, WROWS // 2)
    got("wz_m", wbuf.at[1, u, v], dev_hp)
    send("wzf_m", wbuf.at[1, u, v, lower], wbuf.at[2, u, v, lower], dev_hm)
    got("wz_p", wbuf.at[3, u, v], dev_hm)
    send("wzf_p", wbuf.at[3, u, v, upper], wbuf.at[2, u, v, upper], dev_hp)

    got("buf_p", bbuf.at[v, u2, 0], dev_um)
    got("buf_m", bbuf.at[v, u2, 1], dev_up)
    v_send("b", b_at, u2, 3)

    lane = lax.broadcasted_iota(jnp.int32, (1, BLOCK), 1)
    for j in range(5):
        kept = (lane < len_ref[j]) & (slot_ref[j] >= 0)
        meta_buf[0, j : j + 1, :] = jnp.where(kept, start_ref[j] + lane, -1).astype(F32)
        value = jnp.sum(jnp.where(lane == slot_ref[j], occ_ref[...], 0.0), axis=1, keepdims=True)
        meta_buf[0, 8 + j : 9 + j, :] = jnp.broadcast_to(0.5 - value, (1, BLOCK))
    taking = slot_ref[3] < 0
    meta_buf[0, 5:6, :] = jnp.where(taking, 1.0, 0.0) + jnp.zeros((1, BLOCK), F32)

    send("meta_far", meta_buf.at[0], meta_buf.at[1], dev_far)
    send("meta_mate", meta_buf.at[0], meta_buf.at[2], dev_mate)
    got("meta_far", meta_buf.at[1], dev_far)
    send("meta_mate_far", meta_buf.at[1], meta_buf.at[3], dev_mate)
    got("spare", spare, dev_far)
    own_a[3].wait()
    a_all[6 + c] = jnp.where(taking, spare[...], own3[...])
    send("mate_a3", a_all.at[6 + c], a_all.at[6 + c], dev_mate)

    got("wzf_m", wbuf.at[2, u, v, lower], dev_hp)
    got("wzf_p", wbuf.at[2, u, v, upper], dev_hm)
    send("wu_p", w_at(u, v), w_at(u, v), dev_up)
    send("wu_m", w_at(u, v), w_at(u, v), dev_um)

    for j in range(3):
        own_a[j].wait()
        got(f"mate_a{j}", a_all.at[2 * j + 1 - c], dev_mate)
    got("mate_a3", a_all.at[7 - c], dev_mate)

    left, right = pl.ds(0, BLOCK), pl.ds(BLOCK, BLOCK)

    def compute(k, vk):
        @pl.loop(0, 4)
        def _(d):
            part[k, d] = lax.dot_general(
                bbuf[vk].reshape(CHUNK, bbuf.shape[-1]),
                a_all[pl.ds(2 * d, 2)].reshape(2 * BLOCK, bbuf.shape[-1]),
                (((1,), (1,)), ((), ())),
                preferred_element_type=F32,
            )

        hop_s[k, 0] = part[k, h2, :, left].astype(BF16)
        send(f"hop{k}0", hop_s.at[k, 0], hop_r.at[k, 0], dev_hm)
        hop_s[k, 1] = part[k, h2, :, right].astype(BF16)
        send(f"hop{k}1", hop_s.at[k, 1], hop_r.at[k, 1], dev_hp)
        dir_s[k, 0] = part[k, hm, :, right].astype(BF16)
        send(f"dir{k}0", dir_s.at[k, 0], dir_r.at[k, 0], dev_hm)
        dir_s[k, 1] = part[k, hp, :, left].astype(BF16)
        send(f"dir{k}1", dir_s.at[k, 1], dir_r.at[k, 1], dev_hp)

    def combine(k):
        got(f"hop{k}0", hop_r.at[k, 0], dev_hp)
        comb_s[k, 0] = (part[k, hm, :, left] + hop_r[k, 0].astype(F32)).astype(BF16)
        send(f"comb{k}0", comb_s.at[k, 0], comb_r.at[k, 0], dev_hm)
        got(f"hop{k}1", hop_r.at[k, 1], dev_hm)
        comb_s[k, 1] = (part[k, hp, :, right] + hop_r[k, 1].astype(F32)).astype(BF16)
        send(f"comb{k}1", comb_s.at[k, 1], comb_r.at[k, 1], dev_hp)

    def finish(k, vk):
        got(f"dir{k}0", dir_r.at[k, 0], dev_hp)
        got(f"dir{k}1", dir_r.at[k, 1], dev_hm)
        got(f"comb{k}0", comb_r.at[k, 0], dev_hp)
        got(f"comb{k}1", comb_r.at[k, 1], dev_hm)
        pt[c, vk, :, left] = part[k, h, :, left] + (
            comb_r[k, 0].astype(F32) + dir_r[k, 1].astype(F32)
        )
        pt[c, vk, :, right] = part[k, h, :, right] + (
            comb_r[k, 1].astype(F32) + dir_r[k, 0].astype(F32)
        )
        send(f"pt{k}", pt.at[c, vk], pt.at[c, vk], dev_mate)

    compute(0, v)

    around = (u, um, up, u2)
    for tag in range(4):
        got(f"bv_p{tag}", b_at(around[tag], vm), dev_vm)
        if tag < 2:
            send(f"bvf_p{tag}", b_at(around[tag], vm), b_at(around[tag], vm), dev_vp)
    for tag in range(4):
        got(f"bv_m{tag}", b_at(around[tag], vp), dev_vp)
        if tag >= 2:
            send(f"bvf_m{tag}", b_at(around[tag], vp), b_at(around[tag], vp), dev_vm)

    v_send("w", w_at, u, 0)
    three = pl.ds(1, 3)
    got("wu_p", w_at(um, v), dev_um)
    send("wuf_p", wbuf.at[three, um, v, lower], wbuf.at[three, um, v, lower], dev_up)
    v_send("w", w_at, um, 1)
    got("wu_m", w_at(up, v), dev_up)
    send("wuf_m", wbuf.at[three, up, v, upper], wbuf.at[three, up, v, upper], dev_um)
    v_send("w", w_at, up, 2)

    compute(1, vm)
    combine(0)
    compute(2, vp)
    combine(1)
    finish(0, v)

    got("wuf_p", wbuf.at[three, u2, v, lower], dev_um)
    got("wuf_m", wbuf.at[three, u2, v, upper], dev_up)
    v_send("w", w_at, u2, 3)

    for tag in range(4):
        if tag < 2:
            got(f"bvf_p{tag}", b_at(around[tag], v2), dev_vm)
        else:
            got(f"bvf_m{tag}", b_at(around[tag], v2), dev_vp)
    compute(3, v2)
    combine(2)
    finish(1, vm)
    combine(3)

    for tag in range(4):
        got(f"wv_p{tag}", w_at(around[tag], vm), dev_vm)
        if tag < 2:
            send(f"wvf_p{tag}", w_at(around[tag], vm), w_at(around[tag], vm), dev_vp)
    for tag in range(4):
        got(f"wv_m{tag}", w_at(around[tag], vp), dev_vp)
        if tag >= 2:
            send(f"wvf_m{tag}", w_at(around[tag], vp), w_at(around[tag], vp), dev_vm)

    finish(2, vp)
    finish(3, v2)
    order = (v, vm, vp, v2)
    for k in range(4):
        got(f"pt{k}", pt.at[1 - c, order[k]], dev_mate)

    for src in range(2):
        for vv in range(4):
            for uu in range(4):
                for zz in range(2):
                    xx, yy = (uu, vv) if src == 0 else (vv, uu)
                    first = SHARE * (xx * 16 + zz * 8 + yy * 2 + src)
                    row = PADDED * (2 * uu + zz)
                    ptd[first : first + SHARE, :] = pt[src, vv, row : row + SHARE, :]
    pth[...] = ptd[...].astype(BF16)

    for copy in own_w:
        copy.wait()
    for tag in range(4):
        if tag < 2:
            got(f"wvf_p{tag}", w_at(around[tag], v2), dev_vm)
        else:
            got(f"wvf_m{tag}", w_at(around[tag], v2), dev_vp)

    for q in range(4):
        skip = 128 if q == 3 else 0

        @pl.loop(0, 4)
        def _(rel):
            value = jnp.dot(
                wbuf[rel, :, q, :, skip:].reshape(4 * WROWS, WCOLS - skip),
                pth[WCOLS * q : WCOLS * (q + 1) - skip, :],
                preferred_element_type=F32,
            )
            if q == 0:
                scr[rel] = value
            else:
                scr[rel] += value

    for slot in range(2):
        lanes = pl.ds(slot * BLOCK, BLOCK)
        total = jnp.zeros((BLOCK, BLOCK), F32)
        for rel in range(4):
            base = ((h + rel) % 4) * 736 + c * 368
            for skip, first, count in ((0, 0, 288), (304, 288, 80)):
                rows = pl.ds(pl.multiple_of(base + first, 16), count)
                total += lax.dot_general(
                    scr[rel, pl.ds(skip, count), lanes],
                    ptd[rows, lanes],
                    (((0,), (0,)), ((), ())),
                    preferred_element_type=F32,
                    precision=lax.Precision.HIGHEST,
                )
        bs_own[slot] = total

    send("bs", bs_own, bs_mate, dev_mate)
    got("meta_mate", meta_buf.at[2], dev_mate)
    got("meta_mate_far", meta_buf.at[3], dev_mate)
    item = lax.broadcasted_iota(jnp.int32, (NB_SIGMA // 2, BLOCK), 0)
    rows = (item // 64) * 128 + (item // 8) % 2 * 64 + (item // 16) % 4 * 16 + c * 8 + item % 8
    rows = rows.astype(F32)
    columns = lax.broadcasted_iota(jnp.int32, (NB_SIGMA, BLOCK), 0).astype(F32)
    on_last = h == 3
    places = []
    for slot in range(2):
        own = jnp.where(c == slot, 0, 2)
        swap = (meta_buf[own, 5:6, :] > 0.5) & on_last
        index = jnp.where(swap, meta_buf[own + 1, 4:5, :], meta_buf[own, pl.ds(h, 1), :])
        weight = jnp.where(swap, meta_buf[own + 1, 12:13, :], meta_buf[own, pl.ds(8 + h, 1), :])
        places.append(((rows == index).astype(F32), (columns == index).astype(F32), weight))
    got("bs", bs_mate, dev_mate)
    spread = jnp.zeros((NB_SIGMA // 2, NB_SIGMA), F32)
    for slot in range(2):
        to_rows, to_columns, weight = places[slot]
        wide = lax.dot_general(
            (bs_own[slot] + bs_mate[slot]) * weight,
            to_columns,
            (((1,), (1,)), ((), ())),
            preferred_element_type=F32,
            precision=lax.Precision.HIGHEST,
        )
        spread += jnp.dot(
            to_rows, wide, preferred_element_type=F32, precision=lax.Precision.HIGHEST
        )
    plane_s[...] = spread.astype(BF16).reshape(4, 4, 16, NB_SIGMA)
    for (dx, dy), (place, device) in plane.items():
        send(f"plane{dx}{dy}", plane_s.at[place[0], place[1]], plane_r.at[x, y], device)
    total = plane_s[x, y].astype(F32)
    for dx, dy in plane:
        source = (x + 4 - dx) % 4, (y + 4 - dy) % 4
        landed = plane_r.at[source[0], source[1]]
        got(f"plane{dx}{dy}", landed, plane[(4 - dx) % 4, (4 - dy) % 4][1])
        total += landed[...].astype(F32)
    for zz in range(2):
        for hh in range(4):
            first = 8 * zz + 2 * hh
            line_s[zz, hh] = total[first : first + 2, :]
    for (dz, dh), (place, device) in line.items():
        send(f"line{dz}{dh}", line_s.at[place[0], place[1]], line_r.at[zl, h], device)
    result = line_s[zl, h]
    for dz, dh in line:
        source = (zl + dz) % 2, (h + 4 - dh) % 4
        landed = line_r.at[source[0], source[1]]
        got(f"line{dz}{dh}", landed, line[dz, (4 - dh) % 4][1])
        result += landed[...]
    out_ref[...] = result
    for copy in sent:
        copy.wait_send()
    assert len(ids) <= N_COPIES


def per_device(pair_density, eigvecs, screening, occupation, window_start, window_len, slot_band):
    block, plane_rows = pair_density.shape[1:]
    eig = jnp.pad(eigvecs, ((0, PADDED - SHARE), (0, 0)))
    width = screening.shape[1]
    vmem = pl.BlockSpec(memory_space=pltpu.VMEM)
    hbm = pl.BlockSpec(memory_space=pltpu.HBM)
    scratch = [
        pltpu.VMEM((8, block, plane_rows), BF16),
        pltpu.VMEM((block, plane_rows), BF16),
        pltpu.VMEM((block, plane_rows), BF16),
        pltpu.VMEM((4, 4, 2, PADDED, plane_rows), BF16),
        pltpu.VMEM((4, 4, 4, WROWS, WCOLS), BF16),
        pltpu.VMEM((4, 4, CHUNK, 2 * block), F32),
    ]
    scratch += [pltpu.VMEM((4, 2, CHUNK, block), BF16)] * 6
    scratch += [
        pltpu.VMEM((2, 4, CHUNK, 2 * block), F32),
        pltpu.VMEM((width, 2 * block), F32),
        pltpu.VMEM((width, 2 * block), BF16),
        pltpu.VMEM((4, 4 * WROWS, 2 * block), F32),
        pltpu.VMEM((4, 16, block), F32),
        pltpu.VMEM((2, block, block), F32),
        pltpu.VMEM((2, block, block), F32),
        pltpu.VMEM((4, 4, 16, NB_SIGMA), BF16),
        pltpu.VMEM((4, 4, 16, NB_SIGMA), BF16),
        pltpu.VMEM((2, 4, 2, NB_SIGMA), F32),
        pltpu.VMEM((2, 4, 2, NB_SIGMA), F32),
        pltpu.SemaphoreType.DMA((N_COPIES,)),
        pltpu.SemaphoreType.DMA((N_COPIES,)),
        pltpu.SemaphoreType.DMA((24,)),
    ]
    smem = pl.BlockSpec(memory_space=pltpu.SMEM)
    return pl.pallas_call(
        main_kernel,
        out_shape=jax.ShapeDtypeStruct((2, NB_SIGMA), F32),
        in_specs=[smem, smem, smem, vmem, hbm, hbm, hbm],
        out_specs=vmem,
        scratch_shapes=scratch,
        compiler_params=pltpu.CompilerParams(
            collective_id=0, has_side_effects=True, vmem_limit_bytes=60 * 1024 * 1024
        ),
        name="cohsex",
    )(
        window_start,
        window_len,
        slot_band,
        occupation.reshape(1, -1),
        pair_density,
        eig,
        screening,
    )


def solution(mesh):
    return jax.shard_map(
        per_device,
        mesh=mesh,
        in_specs=(
            P("band", None, "pw"),
            P("band", "pw"),
            P("pw", None),
            P(),
            P("band"),
            P("band"),
            P("band"),
        ),
        out_specs=P(("band", "pw"), None),
        check_vma=False,
    )
```

```python
import jax
import jax.numpy as jnp
from jax import lax
from jax.experimental import pallas as pl
from jax.experimental.pallas import tpu as pltpu
from jax.sharding import PartitionSpec as P

NB_SIGMA = 512
BLOCK = 128
F32 = jnp.float32
BF16 = jnp.bfloat16
HIGHEST = lax.Precision.HIGHEST
SHARE, PADDED = 46, 48
PIECE = 2 * PADDED
CHUNKS = ((0, 4), (4, 6), (6, 10), (10, 12), (12, 16))


def place_of(kv, ku):
    if kv == 0:
        return ku
    return 12 + ku if kv == 3 else 3 + 2 * ku + kv


WROWS, WCOLS = 96, 768
N_COPIES = 200
scope = jax.named_scope


def main_kernel(
    start_ref,
    len_ref,
    slot_ref,
    occ_ref,
    a_ref,
    eig_ref,
    w_ref,
    out_ref,
    a_all,
    spare,
    relay,
    own3,
    bbuf,
    wbuf,
    part,
    hop_s,
    hop_r,
    dir_s,
    dir_r,
    comb_s,
    comb_r,
    pt,
    ptd,
    pth,
    scr,
    meta_buf,
    meta_all,
    bs_own,
    bs_mate,
    plane_s,
    plane_r,
    line_s,
    line_r,
    ssem,
    rsem,
    lsem,
):
    band = lax.axis_index("band")
    h = lax.axis_index("pw")
    x = band // 16
    zl = (band // 8) % 2
    y = (band // 2) % 4
    c = band % 2
    u = x * (1 - c) + y * c
    v = y * (1 - c) + x * c
    su = 16 - 14 * c
    sv = 2 + 14 * c
    hp, hm, h2 = (h + 1) % 4, (h + 3) % 4, (h + 2) % 4
    up, um, u2 = (u + 1) % 4, (u + 3) % 4, (u + 2) % 4
    vp, vm, v2 = (v + 1) % 4, (v + 3) % 4, (v + 2) % 4

    def at_uv(uu, vv):
        return (uu * su + vv * sv + zl * 8 + c, h)

    dev_up, dev_um = at_uv(up, v), at_uv(um, v)
    dev_vp, dev_vm = at_uv(u, vp), at_uv(u, vm)
    dev_hp, dev_hm = (band, hp), (band, hm)
    dev_zl = (x * 16 + (1 - zl) * 8 + y * 2 + c, h)
    dev_mate = (x * 16 + zl * 8 + y * 2 + 1 - c, h)
    dev_far = (((x + 2) % 4) * 16 + zl * 8 + y * 2 + c, h)

    barrier = pltpu.get_barrier_semaphore()
    plane = {}
    for dx in range(4):
        for dy in range(4):
            if dx or dy:
                place = ((x + dx) % 4, (y + dy) % 4)
                plane[dx, dy] = place, (place[0] * 16 + zl * 8 + place[1] * 2 + c, h)
    line = {}
    for dz in range(2):
        for dh in range(4):
            if dz or dh:
                place = ((zl + dz) % 2, (h + dh) % 4)
                line[dz, dh] = place, (x * 16 + place[0] * 8 + y * 2 + c, place[1])
    dev_xp, dev_xm = plane[1, 0][1], plane[3, 0][1]
    peers = [dev_mate] + [device for _, device in [*plane.values(), *line.values()]]
    for peer in peers:
        pl.semaphore_signal(barrier, inc=1, device_id=peer, device_id_type=pl.DeviceIdType.MESH)

    lane = lax.broadcasted_iota(jnp.int32, (1, BLOCK), 1)
    for j in range(5):
        kept = (lane < len_ref[j]) & (slot_ref[j] >= 0)
        meta_buf[0, j : j + 1, :] = jnp.where(kept, start_ref[j] + lane, -1).astype(F32)
        value = jnp.sum(jnp.where(lane == slot_ref[j], occ_ref[...], 0.0), axis=1, keepdims=True)
        meta_buf[0, 8 + j : 9 + j, :] = jnp.broadcast_to(0.5 - value, (1, BLOCK))
    taking = slot_ref[3] < 0
    meta_buf[0, 5:6, :] = jnp.where(taking, 1.0, 0.0) + jnp.zeros((1, BLOCK), F32)
    with scope('barrier'):
        pl.semaphore_wait(barrier, len(peers))

    ids = {}
    sent = []
    sent_by_core = ([], [])

    def remote(name, src, dst, device):
        i = ids.setdefault(name, len(ids))
        return pltpu.make_async_remote_copy(
            src_ref=src,
            dst_ref=dst,
            send_sem=ssem.at[i],
            recv_sem=rsem.at[i],
            device_id=device,
            device_id_type=pl.DeviceIdType.MESH,
        )

    def send(name, src, dst, device, into=sent):
        copy = remote(name, src, dst, device)
        copy.start()
        into.append(copy if into is sent else (name, device))

    def got(name, landing, device):
        with scope("got_" + name):
            remote(name, landing, landing, device).wait_recv()

    local_ids = {}

    def local(name, src, dst):
        i = local_ids.setdefault(name, len(local_ids))
        copy = pltpu.make_async_copy(src, dst, lsem.at[i])
        copy.start()
        return copy

    oz = 1 - zl
    around = (u, um, up, u2)
    order = (v, vm, vp, v2)

    def b_half(kv, ku, zz):
        return bbuf.at[place_of(kv, ku), zz]

    def b_at(kv, ku):
        return bbuf.at[place_of(kv, ku)]

    three = pl.ds(1, 3)
    lower, upper = pl.ds(0, WCOLS // 2), pl.ds(WCOLS // 2, WCOLS // 2)

    def w_at(uu, vv):
        return wbuf.at[three, uu, vv]

    def w_slice(p, q):
        row = pl.multiple_of(c * 368 + p * WROWS - 16 * (p // 3), 16)
        col = pl.multiple_of(q * WCOLS - 128 * (q // 3), 128)
        return w_ref.at[pl.ds(row, WROWS), pl.ds(col, WCOLS)]

    def w_send(uu, tag):
        send(f"wv_p{tag}", w_at(uu, v), w_at(uu, v), dev_vp)
        send(f"wv_m{tag}", w_at(uu, v), w_at(uu, v), dev_vm)

    def b_send(ku):
        send(f"bv_p{ku}", b_at(0, ku), b_at(1, ku), dev_vp)
        send(f"bv_m{ku}", b_at(0, ku), b_at(2, ku), dev_vm)

    def b_got(kv, ku):
        if ku:
            got(f"bv_{'pm'[kv - 1]}{ku}", b_at(kv, ku), dev_vm if kv == 1 else dev_vp)
        else:
            for zz, tag in ((zl, "a"), (oz, "b")):
                device = dev_vm if kv == 1 else dev_vp
                got(f"bv_{'pm'[kv - 1]}0{tag}", b_half(kv, 0, zz), device)

    def far_line(step):
        def core0():
            for kv, ku in (((1, 0),), ((1, 1), (2, 2)), ((2, 3),), ())[step]:
                device = dev_vp if kv == 1 else dev_vm
                send(f"bf{kv}{ku}", b_at(kv, ku), b_at(3, ku), device, sent_by_core[0])
            if step == 3:
                for ku in range(4):
                    got(f"bf{1 if ku < 2 else 2}{ku}", b_at(3, ku), dev_vm if ku < 2 else dev_vp)

        def core1():
            into = sent_by_core[1]
            if step == 0:
                send("bx_p", b_half(1, 0, zl), b_half(3, 0, zl), dev_vp, into)
                send("bx_m", b_half(2, 0, oz), b_half(3, 0, oz), dev_vm, into)
            elif step == 1:
                got("bx_p", b_half(3, 0, zl), dev_vm)
                got("bx_m", b_half(3, 0, oz), dev_vp)
                send("by_p", b_at(3, 0), b_at(3, 1), dev_up, into)
                send("by_m", b_at(3, 0), b_at(3, 2), dev_um, into)
            elif step == 2:
                got("by_p", b_at(3, 1), dev_um)
                send("byf_p", b_half(3, 1, zl), b_half(3, 3, zl), dev_up, into)
                got("by_m", b_at(3, 2), dev_up)
                send("byf_m", b_half(3, 2, oz), b_half(3, 3, oz), dev_um, into)
            else:
                got("byf_p", b_half(3, 3, zl), dev_um)
                got("byf_m", b_half(3, 3, oz), dev_up)

        pl.when(c == 0)(core0)
        pl.when(c == 1)(core1)

    send("zl", eig_ref, b_half(0, 0, zl), dev_zl)
    own_b = local("b", eig_ref, b_half(0, 0, zl))
    send("bu_p0", eig_ref, b_half(0, 1, zl), dev_up)
    send("bu_m0", eig_ref, b_half(0, 2, zl), dev_um)
    send("meta_far", meta_buf.at[0], meta_buf.at[1], dev_far)
    own_a = []
    for j in range(3):
        own_a.append(local(f"a{j}", a_ref.at[j], a_all.at[2 * j + c]))
        send(f"mate_a{j}", a_ref.at[j], a_all.at[2 * j + c], dev_mate)
    own_a.append(local("a3", a_ref.at[3], own3))
    send("bv_p0a", eig_ref, b_half(1, 0, zl), dev_vp)
    send("bv_m0a", eig_ref, b_half(2, 0, zl), dev_vm)

    got("zl", b_half(0, 0, oz), dev_zl)
    send("bu_p1", b_half(0, 0, oz), b_half(0, 1, oz), dev_up)
    send("bu_m1", b_half(0, 0, oz), b_half(0, 2, oz), dev_um)
    send("bv_p0b", b_half(0, 0, oz), b_half(1, 0, oz), dev_vp)
    send("bv_m0b", b_half(0, 0, oz), b_half(2, 0, oz), dev_vm)
    send("wz_m", w_slice(u, v), wbuf.at[1, u, v], dev_hm)
    send("wz_p", w_slice(u, v), wbuf.at[3, u, v], dev_hp)

    got("bu_p0", b_half(0, 1, zl), dev_um)
    send("buf_p", b_half(0, 1, zl), b_half(0, 3, zl), dev_up)
    got("bu_m0", b_half(0, 2, zl), dev_up)
    got("bu_m1", b_half(0, 2, oz), dev_up)
    send("buf_m", b_half(0, 2, oz), b_half(0, 3, oz), dev_um)
    near, far = pl.ds(0, BLOCK // 2), pl.ds(BLOCK // 2, BLOCK // 2)
    send("spare_p", a_ref.at[4, near], relay.at[0], dev_xp)
    send("spare_m", a_ref.at[4, far], relay.at[1], dev_xm)
    got("bu_p1", b_half(0, 1, oz), dev_um)
    b_send(1)
    b_send(2)
    got("wz_m", wbuf.at[1, u, v], dev_hp)
    send("wzf_m", wbuf.at[1, u, v, :, lower], wbuf.at[2, u, v, :, lower], dev_hm)
    got("wz_p", wbuf.at[3, u, v], dev_hm)
    send("wzf_p", wbuf.at[3, u, v, :, upper], wbuf.at[2, u, v, :, upper], dev_hp)
    own_b.wait()
    for j in range(3):
        own_a[j].wait()
        got(f"mate_a{j}", a_all.at[2 * j + 1 - c], dev_mate)
    got("buf_p", b_half(0, 3, zl), dev_um)
    got("buf_m", b_half(0, 3, oz), dev_up)

    def slot_of(r, cc):
        return (h + r + 7 - 2 * cc - zl) % 4

    def half(cc):
        return pl.ds(cc * BLOCK, BLOCK)

    def project(k, j):
        lo, hi = CHUNKS[k]
        rows = (hi - lo) * PIECE
        part[j, lo:hi] = lax.dot_general(
            bbuf[lo:hi].reshape(rows, bbuf.shape[-1]),
            a_all[pl.ds(2 * j, 2)].reshape(2 * BLOCK, bbuf.shape[-1]),
            (((1,), (1,)), ((), ())),
            preferred_element_type=F32,
        ).reshape(hi - lo, PIECE, 2 * BLOCK)

    def span(k):
        return pl.ds(CHUNKS[k][0], CHUNKS[k][1] - CHUNKS[k][0])

    def phase(late, j, run):
        pl.when((j == 3) if late else (j != 3))(run)

    def compute(k, late):
        with scope(f"compute{k}_{late}"):
            if late:
                project(k, 3)
            else:

                @pl.loop(0, 3)
                def _(j):
                    project(k, j)

            for name, i, r, cc, send_buf, recv_buf, device in (
                ("hop", 0, 2, 0, hop_s, hop_r, dev_hm),
                ("hop", 1, 2, 1, hop_s, hop_r, dev_hp),
                ("dir", 0, 3, 1, dir_s, dir_r, dev_hm),
                ("dir", 1, 1, 0, dir_s, dir_r, dev_hp),
            ):
                j = slot_of(r, cc)
                copy = remote(
                    f"{name}{k}{i}", send_buf.at[i, span(k)], recv_buf.at[i, span(k)], device
                )
                if not late:
                    sent.append(copy)

                def run():
                    send_buf[i, span(k)] = part[j, span(k), :, half(cc)].astype(BF16)
                    copy.start()

                phase(late, j, run)

    def combine(k, late, core=None):
        for i, r, cc, source, device in ((0, 3, 0, dev_hp, dev_hm), (1, 1, 1, dev_hm, dev_hp)):
            j = slot_of(r, cc)
            copy = remote(
                f"comb{k}{i}", comb_s.at[i, span(k)], comb_r.at[i, span(k)], device
            )
            if not late and core != 1:
                sent.append(copy)

            def run():
                got(f"hop{k}{i}", hop_r.at[i, span(k)], source)
                total = part[j, span(k), :, half(cc)] + hop_r[i, span(k)].astype(F32)
                comb_s[i, span(k)] = total.astype(BF16)
                copy.start()

            if core is None:
                phase(late, j, run)
            else:
                pl.when((j != 3) & (c == core))(run)

    def finish(k, late):
        for cc, first, second in ((0, dev_hp, dev_hm), (1, dev_hm, dev_hp)):
            j = slot_of(0, cc)
            mine = pt.at[c, cc, span(k)]
            to_mate = remote(f"pt{k}{cc}", mine, mine, dev_mate)
            if not late:
                sent.append(to_mate)

            def run():
                got(f"dir{k}{1 - cc}", dir_r.at[1 - cc, span(k)], second)
                got(f"comb{k}{cc}", comb_r.at[cc, span(k)], first)
                pt[c, cc, span(k)] = part[j, span(k), :, half(cc)] + (
                    comb_r[cc, span(k)].astype(F32) + dir_r[1 - cc, span(k)].astype(F32)
                )
                to_mate.start()

            phase(late, j, run)

    compute(0, False)

    got("meta_far", meta_buf.at[1], dev_far)
    swap = meta_buf[0, 5:6, :] > 0.5
    for row, far_row in ((0, 4), (8, 12)):
        first = row // 2
        meta_all[c, first : first + 3, :] = meta_buf[0, row : row + 3, :]
        meta_all[c, first + 3 : first + 4, :] = jnp.where(
            swap, meta_buf[1, far_row : far_row + 1, :], meta_buf[0, row + 3 : row + 4, :]
        )
    send("meta_mate", meta_all.at[c], meta_all.at[c], dev_mate)

    b_got(1, 0)
    b_got(2, 0)
    far_line(0)
    compute(1, False)
    got("spare_p", relay.at[0], dev_xm)
    send("spare_pf", relay.at[0], spare.at[near], dev_xp)
    got("spare_m", relay.at[1], dev_xp)
    send("spare_mf", relay.at[1], spare.at[far], dev_xm)
    b_send(3)
    combine(0, False, 1)
    b_got(1, 1)
    b_got(2, 1)
    b_got(2, 2)
    b_got(1, 2)
    far_line(1)
    compute(2, False)
    combine(0, False, 0)
    combine(1, False)

    got("wzf_m", wbuf.at[2, u, v, :, lower], dev_hp)
    got("wzf_p", wbuf.at[2, u, v, :, upper], dev_hm)
    send("wu_p", w_at(u, v), w_at(u, v), dev_up)
    send("wu_m", w_at(u, v), w_at(u, v), dev_um)
    w_send(u, 0)
    own_w = []
    for p in range(4):
        for q in range(4):
            own_w.append(local(f"w{p}{q}", w_slice(p, q), wbuf.at[0, p, q]))

    got("spare_pf", spare.at[near], dev_xm)
    got("spare_mf", spare.at[far], dev_xp)
    own_a[3].wait()
    a_all[6 + c] = jnp.where(taking, spare[...], own3[...])
    send("mate_a3", a_all.at[6 + c], a_all.at[6 + c], dev_mate)
    got("mate_a3", a_all.at[7 - c], dev_mate)
    compute(0, True)
    compute(1, True)
    compute(2, True)
    combine(2, False)
    b_got(2, 3)
    b_got(1, 3)
    far_line(2)
    compute(3, False)
    compute(3, True)

    got("wu_p", w_at(um, v), dev_um)
    send(
        "wuf_p", wbuf.at[three, um, v, :, lower], wbuf.at[three, um, v, :, lower], dev_up
    )
    w_send(um, 1)
    got("wu_m", w_at(up, v), dev_up)
    send(
        "wuf_m", wbuf.at[three, up, v, :, upper], wbuf.at[three, up, v, :, upper], dev_um
    )
    w_send(up, 2)
    combine(0, True)
    combine(1, True)
    far_line(3)
    compute(4, False)
    compute(4, True)
    combine(2, True)
    combine(3, False)
    combine(3, True)
    got("wuf_p", wbuf.at[three, u2, v, :, lower], dev_um)
    got("wuf_m", wbuf.at[three, u2, v, :, upper], dev_up)
    w_send(u2, 3)
    got("wv_p0", w_at(u, vm), dev_vm)
    send("wvf_p0", w_at(u, vm), w_at(u, vm), dev_vp)
    got("wv_p1", w_at(um, vm), dev_vm)
    send("wvf_p1", w_at(um, vm), w_at(um, vm), dev_vp)
    combine(4, False)
    got("wv_m0", w_at(u, vp), dev_vp)
    got("wv_m1", w_at(um, vp), dev_vp)
    got("wv_m2", w_at(up, vp), dev_vp)
    send("wvf_m2", w_at(up, vp), w_at(up, vp), dev_vm)
    combine(4, True)
    got("wv_m3", w_at(u2, vp), dev_vp)
    send("wvf_m3", w_at(u2, vp), w_at(u2, vp), dev_vm)
    got("wv_p2", w_at(up, vm), dev_vm)
    got("wv_p3", w_at(u2, vm), dev_vm)
    for k in range(5):
        finish(k, False)
        finish(k, True)
    for k in range(5):
        for cc in range(2):
            got(f"pt{k}{cc}", pt.at[1 - c, cc, span(k)], dev_mate)

    def rank(there, here):
        step = (2 * ((there + 4 - here) % 4)) % 5
        return step - step // 4

    with scope("assemble"):
        for src in range(2):
            own = c == src
            u_src, v_src = jnp.where(own, u, v), jnp.where(own, v, u)
            for vv in range(4):
                kv = rank(vv, v_src)
                for uu in range(4):
                    ku = rank(uu, u_src)
                    place = jnp.where(kv == 3, 12 + ku, 3 + 2 * ku + kv)
                    place = jnp.where(kv == 0, ku, place)
                    for zz in range(2):
                        xx, yy = (uu, vv) if src == 0 else (vv, uu)
                        first = SHARE * (xx * 16 + zz * 8 + yy * 2 + src)
                        row = PADDED * zz
                        for cc in range(2):
                            ptd[first : first + SHARE, half(cc)] = pt[
                                src, cc, place, row : row + SHARE, :
                            ]
        for q in range(3):
            pth[q] = ptd[q * WCOLS : (q + 1) * WCOLS, :].astype(BF16)
        pth[3, :128] = jnp.zeros((128, 2 * BLOCK), BF16)
        pth[3, 128:] = ptd[3 * WCOLS :, :].astype(BF16)

    def screen(k, q):
        with scope(f"screen{k}"):

            @pl.loop(0, 2)
            def _(n):
                two = pl.ds(2 * n, 2)
                rows = pl.ds(pl.multiple_of(n * 8 * WROWS, 8 * WROWS), 8 * WROWS)
                value = jnp.dot(
                    wbuf[two, :, q].reshape(8 * WROWS, WCOLS),
                    pth[q],
                    preferred_element_type=F32,
                )
                if k == 0:
                    scr[rows, :] = value
                else:
                    scr[rows, :] += value

    for copy in own_w:
        copy.wait()
    screen(0, v)
    screen(1, vm)
    screen(2, vp)
    for tag in range(4):
        if tag < 2:
            got(f"wvf_p{tag}", w_at(around[tag], v2), dev_vm)
        else:
            got(f"wvf_m{tag}", w_at(around[tag], v2), dev_vp)
    screen(3, v2)
    with scope("bs"):
        for slot in range(2):
            total = jnp.zeros((BLOCK, BLOCK), F32)
            for rel in range(4):
                base = ((h + rel) % 4) * 736 + c * 368
                for skip, first, count in ((0, 0, 288), (304, 288, 80)):
                    total += lax.dot_general(
                        scr[pl.ds(rel * 4 * WROWS + skip, count), half(slot)],
                        ptd[pl.ds(pl.multiple_of(base + first, 16), count), half(slot)],
                        (((0,), (0,)), ((), ())),
                        preferred_element_type=F32,
                        precision=HIGHEST,
                    )
            bs_own[slot] = total
    send("bs", bs_own, bs_mate, dev_mate)

    got("meta_mate", meta_all.at[1 - c], dev_mate)
    with scope("places"):
        item = lax.broadcasted_iota(jnp.int32, (NB_SIGMA // 2, BLOCK), 0)
        rows = (item // 64) * 128 + (item // 8) % 2 * 64 + (item // 16) % 4 * 16 + c * 8 + item % 8
        rows = rows.astype(F32)
        columns = lax.broadcasted_iota(jnp.int32, (NB_SIGMA, BLOCK), 0).astype(F32)
        places = []
        for cc in range(2):
            j = slot_of(0, cc)
            index = meta_all[cc, pl.ds(j, 1), :]
            weight = meta_all[cc, pl.ds(4 + j, 1), :]
            places.append(((rows == index).astype(BF16), (columns == index).astype(BF16), weight))
    got("bs", bs_mate, dev_mate)
    with scope("spread"):
        spread = jnp.zeros((NB_SIGMA // 2, NB_SIGMA), F32)
        for slot in range(2):
            to_rows, to_columns, weight = places[slot]
            block = (bs_own[slot] + bs_mate[slot]) * weight
            high = block.astype(BF16)
            low = (block - high.astype(F32)).astype(BF16)
            for term in (high, low):
                wide = lax.dot_general(
                    term, to_columns, (((1,), (1,)), ((), ())), preferred_element_type=F32
                )
                spread += jnp.dot(to_rows, wide.astype(BF16), preferred_element_type=F32)
        plane_s[...] = spread.astype(BF16).reshape(4, 4, 16, NB_SIGMA)
    for (dx, dy), (place, device) in plane.items():
        send(f"plane{dx}{dy}", plane_s.at[place[0], place[1]], plane_r.at[x, y], device)
    total = plane_s[x, y].astype(F32)
    for dx, dy in plane:
        source = (x + 4 - dx) % 4, (y + 4 - dy) % 4
        landed = plane_r.at[source[0], source[1]]
        got(f"plane{dx}{dy}", landed, plane[(4 - dx) % 4, (4 - dy) % 4][1])
        total += landed[...].astype(F32)
    for zz in range(2):
        for hh in range(4):
            first = 8 * zz + 2 * hh
            line_s[zz, hh] = total[first : first + 2, :]
    for (dz, dh), (place, device) in line.items():
        send(f"line{dz}{dh}", line_s.at[place[0], place[1]], line_r.at[zl, h], device)
    result = line_s[zl, h]
    for dz, dh in line:
        source = (zl + dz) % 2, (h + 4 - dh) % 4
        landed = line_r.at[source[0], source[1]]
        got(f"line{dz}{dh}", landed, line[dz, (4 - dh) % 4][1])
        result += landed[...]
    out_ref[...] = result
    for copy in sent:
        copy.wait_send()
    for core in range(2):

        @pl.when(c == core)
        def _():
            for name, device in sent_by_core[core]:
                whole = core == 0 or name in ("by_p", "by_m")
                piece = b_at(0, 0) if whole else b_half(0, 0, 0)
                remote(name, piece, piece, device).wait_send()

    assert len(ids) <= N_COPIES


def per_device(pair_density, eigvecs, screening, occupation, window_start, window_len, slot_band):
    block, plane_rows = pair_density.shape[1:]
    eig = jnp.pad(eigvecs, ((0, PADDED - SHARE), (0, 0)))
    width = screening.shape[1]
    vmem = pl.BlockSpec(memory_space=pltpu.VMEM)
    hbm = pl.BlockSpec(memory_space=pltpu.HBM)
    scratch = [
        pltpu.VMEM((8, block, plane_rows), BF16),
        pltpu.VMEM((block, plane_rows), BF16),
        pltpu.VMEM((2, block // 2, plane_rows), BF16),
        pltpu.VMEM((block, plane_rows), BF16),
        pltpu.VMEM((16, 2, PADDED, plane_rows), BF16),
        pltpu.VMEM((4, 4, 4, WROWS, WCOLS), BF16),
        pltpu.VMEM((4, 16, PIECE, 2 * block), F32),
    ]
    scratch += [pltpu.VMEM((2, 16, PIECE, block), BF16)] * 6
    scratch += [
        pltpu.VMEM((2, 2, 16, PIECE, block), F32),
        pltpu.VMEM((width, 2 * block), F32),
        pltpu.VMEM((4, WCOLS, 2 * block), BF16),
        pltpu.VMEM((16 * WROWS, 2 * block), F32),
        pltpu.VMEM((2, 16, block), F32),
        pltpu.VMEM((2, 8, block), F32),
        pltpu.VMEM((2, block, block), F32),
        pltpu.VMEM((2, block, block), F32),
        pltpu.VMEM((4, 4, 16, NB_SIGMA), BF16),
        pltpu.VMEM((4, 4, 16, NB_SIGMA), BF16),
        pltpu.VMEM((2, 4, 2, NB_SIGMA), F32),
        pltpu.VMEM((2, 4, 2, NB_SIGMA), F32),
        pltpu.SemaphoreType.DMA((N_COPIES,)),
        pltpu.SemaphoreType.DMA((N_COPIES,)),
        pltpu.SemaphoreType.DMA((24,)),
    ]
    smem = pl.BlockSpec(memory_space=pltpu.SMEM)
    return pl.pallas_call(
        main_kernel,
        out_shape=jax.ShapeDtypeStruct((2, NB_SIGMA), F32),
        in_specs=[smem, smem, smem, vmem, hbm, hbm, hbm],
        out_specs=vmem,
        scratch_shapes=scratch,
        compiler_params=pltpu.CompilerParams(
            collective_id=0, has_side_effects=True, vmem_limit_bytes=60 * 1024 * 1024
        ),
        name="cohsex",
    )(
        window_start,
        window_len,
        slot_band,
        occupation.reshape(1, -1),
        pair_density,
        eig,
        screening,
    )


def solution(mesh):
    return jax.shard_map(
        per_device,
        mesh=mesh,
        in_specs=(
            P("band", None, "pw"),
            P("band", "pw"),
            P("pw", None),
            P(),
            P("band"),
            P("band"),
            P("band"),
        ),
        out_specs=P(("band", "pw"), None),
        check_vma=False,
    )
```

```python
import jax
import jax.numpy as jnp
from jax import lax
from jax.experimental import pallas as pl
from jax.experimental.pallas import tpu as pltpu
from jax.sharding import PartitionSpec as P

NB_SIGMA = 512
BLOCK = 128
F32 = jnp.float32
BF16 = jnp.bfloat16
HIGHEST = lax.Precision.HIGHEST
SHARE, PADDED = 46, 48
PIECE = 2 * PADDED
CHUNKS = ((0, 4), (4, 6), (6, 8), (8, 10), (10, 12), (12, 16))


def place_of(kv, ku):
    if kv == 0:
        return ku
    return 12 + ku if kv == 3 else 3 + 2 * ku + kv


WROWS, WCOLS = 96, 768
N_COPIES = 220
scope = jax.named_scope


def main_kernel(
    start_ref,
    len_ref,
    slot_ref,
    occ_ref,
    a_ref,
    eig_ref,
    w_ref,
    out_ref,
    a_all,
    spare,
    relay,
    own3,
    share,
    bbuf,
    wbuf,
    part,
    hop_s,
    hop_r,
    dir_s,
    dir_r,
    comb_s,
    comb_r,
    pt,
    ptd,
    pth,
    ptd_h,
    ptd_l,
    scr_h,
    scr_l,
    meta_buf,
    meta_all,
    bs_own,
    bs_mate,
    plane_s,
    plane_r,
    line_s,
    line_r,
    ssem,
    rsem,
    lsem,
):
    band = lax.axis_index("band")
    h = lax.axis_index("pw")
    x = band // 16
    zl = (band // 8) % 2
    y = (band // 2) % 4
    c = band % 2
    u = x * (1 - c) + y * c
    v = y * (1 - c) + x * c
    su = 16 - 14 * c
    sv = 2 + 14 * c
    hp, hm, h2 = (h + 1) % 4, (h + 3) % 4, (h + 2) % 4
    up, um, u2 = (u + 1) % 4, (u + 3) % 4, (u + 2) % 4
    vp, vm, v2 = (v + 1) % 4, (v + 3) % 4, (v + 2) % 4

    def at_uv(uu, vv):
        return (uu * su + vv * sv + zl * 8 + c, h)

    dev_up, dev_um = at_uv(up, v), at_uv(um, v)
    dev_vp, dev_vm = at_uv(u, vp), at_uv(u, vm)
    dev_hp, dev_hm = (band, hp), (band, hm)
    dev_zl = (x * 16 + (1 - zl) * 8 + y * 2 + c, h)
    dev_mate = (x * 16 + zl * 8 + y * 2 + 1 - c, h)
    dev_far = (((x + 2) % 4) * 16 + zl * 8 + y * 2 + c, h)

    barrier = pltpu.get_barrier_semaphore()
    plane = {}
    for dx in range(4):
        for dy in range(4):
            if dx or dy:
                place = ((x + dx) % 4, (y + dy) % 4)
                plane[dx, dy] = place, (place[0] * 16 + zl * 8 + place[1] * 2 + c, h)
    line = {}
    for dz in range(2):
        for dh in range(4):
            if dz or dh:
                place = ((zl + dz) % 2, (h + dh) % 4)
                line[dz, dh] = place, (x * 16 + place[0] * 8 + y * 2 + c, place[1])
    dev_xp, dev_xm = plane[1, 0][1], plane[3, 0][1]
    peers = [dev_mate, dev_up, dev_um, dev_vp, dev_vm, dev_hp, dev_hm, dev_zl, dev_far]
    for peer in peers:
        pl.semaphore_signal(barrier, inc=1, device_id=peer, device_id_type=pl.DeviceIdType.MESH)

    own_b = pltpu.make_async_copy(eig_ref, share, lsem.at[23])
    own_b.start()
    lane = lax.broadcasted_iota(jnp.int32, (1, BLOCK), 1)
    for j in range(5):
        kept = (lane < len_ref[j]) & (slot_ref[j] >= 0)
        meta_buf[0, j : j + 1, :] = jnp.where(kept, start_ref[j] + lane, -1).astype(F32)
        value = jnp.sum(jnp.where(lane == slot_ref[j], occ_ref[...], 0.0), axis=1, keepdims=True)
        meta_buf[0, 8 + j : 9 + j, :] = jnp.broadcast_to(0.5 - value, (1, BLOCK))
    taking = slot_ref[3] < 0
    meta_buf[0, 5:6, :] = jnp.where(taking, 1.0, 0.0) + jnp.zeros((1, BLOCK), F32)
    own_b.wait()
    bbuf[0, zl, :SHARE] = share[...]
    bbuf[0, zl, SHARE:] = jnp.zeros((PADDED - SHARE, share.shape[1]), BF16)
    with scope('barrier'):
        pl.semaphore_wait(barrier, len(peers))

    ids = {}
    sent = []
    sent_by_core = ([], [])
    pieces = {}

    def remote(name, src, dst, device):
        i = ids.setdefault(name, len(ids))
        return pltpu.make_async_remote_copy(
            src_ref=src,
            dst_ref=dst,
            send_sem=ssem.at[i],
            recv_sem=rsem.at[i],
            device_id=device,
            device_id_type=pl.DeviceIdType.MESH,
        )

    def send(name, src, dst, device, into=sent):
        copy = remote(name, src, dst, device)
        copy.start()
        into.append(copy if into is sent else (name, device))

    def got(name, landing, device):
        with scope("got_" + name):
            remote(name, landing, landing, device).wait_recv()

    local_ids = {}

    def local(name, src, dst):
        i = local_ids.setdefault(name, len(local_ids))
        copy = pltpu.make_async_copy(src, dst, lsem.at[i])
        copy.start()
        return copy

    oz = 1 - zl
    around = (u, um, up, u2)
    order = (v, vm, vp, v2)

    def b_half(kv, ku, zz):
        return bbuf.at[place_of(kv, ku), zz]

    def b_at(kv, ku):
        return bbuf.at[place_of(kv, ku)]

    three = pl.ds(1, 3)
    lower, upper = pl.ds(0, WCOLS // 2), pl.ds(WCOLS // 2, WCOLS // 2)

    def w_at(uu, vv):
        return wbuf.at[three, uu, vv]

    def w_slice(p, q):
        row = pl.multiple_of(c * 368 + p * WROWS - 16 * (p // 3), 16)
        col = pl.multiple_of(q * WCOLS - 128 * (q // 3), 128)
        return w_ref.at[pl.ds(row, WROWS), pl.ds(col, WCOLS)]

    def w_send(uu, tag):
        send(f"wv_p{tag}", w_at(uu, v), w_at(uu, v), dev_vp)
        send(f"wv_m{tag}", w_at(uu, v), w_at(uu, v), dev_vm)

    def b_send(ku):
        for name, kv, device in ((f"bv_p{ku}", 1, dev_vp), (f"bv_m{ku}", 2, dev_vm)):
            remote(name, b_at(0, ku), b_at(kv, ku), device).start()
            pieces[name] = device

    def b_got(kv, ku):
        if ku:
            got(f"bv_{'pm'[kv - 1]}{ku}", b_at(kv, ku), dev_vm if kv == 1 else dev_vp)
        else:
            for zz, tag in ((zl, "a"), (oz, "b")):
                device = dev_vm if kv == 1 else dev_vp
                got(f"bv_{'pm'[kv - 1]}0{tag}", b_half(kv, 0, zz), device)

    def far_line(step, core=None):
        def core0():
            for kv, ku in (((1, 0),), ((1, 1),), ((2, 2),), ((2, 3),), ())[step]:
                device = dev_vp if kv == 1 else dev_vm
                send(f"bf{kv}{ku}", b_at(kv, ku), b_at(3, ku), device, sent_by_core[0])
            if step == 4:
                for ku in range(4):
                    got(f"bf{1 if ku < 2 else 2}{ku}", b_at(3, ku), dev_vm if ku < 2 else dev_vp)

        def core1():
            into = sent_by_core[1]
            if step == 0:
                send("bx_p", b_half(1, 0, zl), b_half(3, 0, zl), dev_vp, into)
                send("bx_m", b_half(2, 0, oz), b_half(3, 0, oz), dev_vm, into)
            elif step == 1:
                pass
            elif step == 2:
                got("bx_p", b_half(3, 0, zl), dev_vm)
                got("bx_m", b_half(3, 0, oz), dev_vp)
                send("by_p", b_at(3, 0), b_at(3, 1), dev_up, into)
                send("by_m", b_at(3, 0), b_at(3, 2), dev_um, into)
            elif step == 3:
                got("by_p", b_at(3, 1), dev_um)
                send("byf_p", b_half(3, 1, zl), b_half(3, 3, zl), dev_up, into)
                got("by_m", b_at(3, 2), dev_up)
                send("byf_m", b_half(3, 2, oz), b_half(3, 3, oz), dev_um, into)
            else:
                got("byf_p", b_half(3, 3, zl), dev_um)
                got("byf_m", b_half(3, 3, oz), dev_up)

        if core != 1:
            pl.when(c == 0)(core0)
        if core != 0:
            pl.when(c == 1)(core1)

    send("zl", b_half(0, 0, zl), b_half(0, 0, zl), dev_zl)
    send("bu_p0", b_half(0, 0, zl), b_half(0, 1, zl), dev_up)
    send("bu_m0", b_half(0, 0, zl), b_half(0, 2, zl), dev_um)
    send("meta_far", meta_buf.at[0], meta_buf.at[1], dev_far)
    own_a = []
    for j in range(3):
        own_a.append(local(f"a{j}", a_ref.at[j], a_all.at[2 * j + c]))
        send(f"mate_a{j}", a_ref.at[j], a_all.at[2 * j + c], dev_mate)
    own_a.append(local("a3", a_ref.at[3], own3))
    send("bv_p0a", b_half(0, 0, zl), b_half(1, 0, zl), dev_vp)
    send("bv_m0a", b_half(0, 0, zl), b_half(2, 0, zl), dev_vm)

    got("zl", b_half(0, 0, oz), dev_zl)
    send("bu_p1", b_half(0, 0, oz), b_half(0, 1, oz), dev_up)
    send("bu_m1", b_half(0, 0, oz), b_half(0, 2, oz), dev_um)
    send("bv_p0b", b_half(0, 0, oz), b_half(1, 0, oz), dev_vp)
    send("bv_m0b", b_half(0, 0, oz), b_half(2, 0, oz), dev_vm)
    send("wz_m", w_slice(u, v), wbuf.at[1, u, v], dev_hm)
    send("wz_p", w_slice(u, v), wbuf.at[3, u, v], dev_hp)

    got("bu_p0", b_half(0, 1, zl), dev_um)
    send("buf_p", b_half(0, 1, zl), b_half(0, 3, zl), dev_up)
    got("bu_m0", b_half(0, 2, zl), dev_up)
    got("bu_m1", b_half(0, 2, oz), dev_up)
    send("buf_m", b_half(0, 2, oz), b_half(0, 3, oz), dev_um)
    near, far = pl.ds(0, BLOCK // 2), pl.ds(BLOCK // 2, BLOCK // 2)
    send("spare_p", a_ref.at[4, near], relay.at[0], dev_xp)
    send("spare_m", a_ref.at[4, far], relay.at[1], dev_xm)
    got("bu_p1", b_half(0, 1, oz), dev_um)
    b_send(1)
    pl.when(c == 0)(lambda: b_send(2))
    got("wz_m", wbuf.at[1, u, v], dev_hp)
    send("wzf_m", wbuf.at[1, u, v, :, lower], wbuf.at[2, u, v, :, lower], dev_hm)
    got("wz_p", wbuf.at[3, u, v], dev_hm)
    send("wzf_p", wbuf.at[3, u, v, :, upper], wbuf.at[2, u, v, :, upper], dev_hp)
    for j in range(3):
        own_a[j].wait()
        got(f"mate_a{j}", a_all.at[2 * j + 1 - c], dev_mate)
    got("buf_p", b_half(0, 3, zl), dev_um)
    got("buf_m", b_half(0, 3, oz), dev_up)

    def slot_of(r, cc):
        return (h + r + 7 - 2 * cc - zl) % 4

    def half(cc):
        return pl.ds(cc * BLOCK, BLOCK)

    def project(k, j):
        lo, hi = CHUNKS[k]
        rows = (hi - lo) * PIECE
        part[j, lo:hi] = lax.dot_general(
            bbuf[lo:hi].reshape(rows, bbuf.shape[-1]),
            a_all[pl.ds(2 * j, 2)].reshape(2 * BLOCK, bbuf.shape[-1]),
            (((1,), (1,)), ((), ())),
            preferred_element_type=F32,
        ).reshape(hi - lo, PIECE, 2 * BLOCK)

    def span(k):
        return pl.ds(CHUNKS[k][0], CHUNKS[k][1] - CHUNKS[k][0])

    chunks_sent = {}

    def phase(late, j, run):
        pl.when((j == 3) if late else (j != 3))(run)

    def compute(k, late):
        with scope(f"compute{k}_{late}"):
            if late:
                project(k, 3)
            else:

                @pl.loop(0, 3)
                def _(j):
                    project(k, j)

            for name, i, r, cc, send_buf, recv_buf, device in (
                ("hop", 0, 2, 0, hop_s, hop_r, dev_hm),
                ("hop", 1, 2, 1, hop_s, hop_r, dev_hp),
                ("dir", 0, 3, 1, dir_s, dir_r, dev_hm),
                ("dir", 1, 1, 0, dir_s, dir_r, dev_hp),
            ):
                j = slot_of(r, cc)
                copy = remote(
                    f"{name}{k}{i}", send_buf.at[i, span(k)], recv_buf.at[i, span(k)], device
                )
                chunks_sent[f"{name}{k}{i}"] = (f"{name}{k}{i}", k, i, device)

                def run():
                    send_buf[i, span(k)] = part[j, span(k), :, half(cc)].astype(BF16)
                    copy.start()

                phase(late, j, run)

    def combine(k, late, core=None):
        for i, r, cc, source, device in ((0, 3, 0, dev_hp, dev_hm), (1, 1, 1, dev_hm, dev_hp)):
            j = slot_of(r, cc)
            copy = remote(
                f"comb{k}{i}", comb_s.at[i, span(k)], comb_r.at[i, span(k)], device
            )
            chunks_sent[f"comb{k}{i}"] = (f"comb{k}{i}", k, i, device)

            def run():
                got(f"hop{k}{i}", hop_r.at[i, span(k)], source)
                total = part[j, span(k), :, half(cc)] + hop_r[i, span(k)].astype(F32)
                comb_s[i, span(k)] = total.astype(BF16)
                copy.start()

            if core is None:
                phase(late, j, run)
            else:
                pl.when((j != 3) & (c == core))(run)

    def finish(k, late):
        for cc, first, second in ((0, dev_hp, dev_hm), (1, dev_hm, dev_hp)):
            j = slot_of(0, cc)
            mine = pt.at[c, cc, span(k)]
            to_mate = remote(f"pt{k}{cc}", mine, mine, dev_mate)
            if not late:
                sent.append(to_mate)

            def run():
                got(f"dir{k}{1 - cc}", dir_r.at[1 - cc, span(k)], second)
                got(f"comb{k}{cc}", comb_r.at[cc, span(k)], first)
                pt[c, cc, span(k)] = part[j, span(k), :, half(cc)] + (
                    comb_r[cc, span(k)].astype(F32) + dir_r[1 - cc, span(k)].astype(F32)
                )
                to_mate.start()

            phase(late, j, run)

    compute(0, False)

    got("meta_far", meta_buf.at[1], dev_far)
    swap = meta_buf[0, 5:6, :] > 0.5
    for row, far_row in ((0, 4), (8, 12)):
        first = row // 2
        meta_all[c, first : first + 3, :] = meta_buf[0, row : row + 3, :]
        meta_all[c, first + 3 : first + 4, :] = jnp.where(
            swap, meta_buf[1, far_row : far_row + 1, :], meta_buf[0, row + 3 : row + 4, :]
        )
    send("meta_mate", meta_all.at[c], meta_all.at[c], dev_mate)

    b_got(1, 0)
    b_got(2, 0)
    far_line(0)
    compute(1, False)
    got("spare_p", relay.at[0], dev_xm)
    send("spare_pf", relay.at[0], spare.at[near], dev_xp)
    got("spare_m", relay.at[1], dev_xp)
    send("spare_mf", relay.at[1], spare.at[far], dev_xm)
    pl.when(c == 1)(lambda: b_send(2))
    b_send(3)
    combine(0, False, 1)
    b_got(1, 1)
    far_line(1)
    b_got(2, 1)
    compute(2, False)
    combine(0, False, 0)
    b_got(2, 2)
    b_got(1, 2)
    far_line(2)
    compute(3, False)
    combine(1, False)

    def fifth(core):
        b_got(2, 3)
        far_line(3, core)
        b_got(1, 3)
        compute(4, False)

    @pl.when(c == 0)
    def _():
        fifth(0)
        combine(2, False)

    got("wzf_m", wbuf.at[2, u, v, :, lower], dev_hp)
    got("wzf_p", wbuf.at[2, u, v, :, upper], dev_hm)
    send("wu_p", w_at(u, v), w_at(u, v), dev_up)
    send("wu_m", w_at(u, v), w_at(u, v), dev_um)
    own_w = []
    for p in range(4):
        for q in range(4):
            own_w.append(local(f"w{p}{q}", w_slice(p, q), wbuf.at[0, p, q]))

    got("spare_pf", spare.at[near], dev_xm)
    got("spare_mf", spare.at[far], dev_xp)
    own_a[3].wait()
    a_all[6 + c] = jnp.where(taking, spare[...], own3[...])
    send("mate_a3", a_all.at[6 + c], a_all.at[6 + c], dev_mate)
    got("mate_a3", a_all.at[7 - c], dev_mate)
    for k in range(4):
        compute(k, True)
    combine(2, False, 1)
    combine(3, False)
    pl.when(c == 1)(lambda: fifth(1))
    w_send(u, 0)
    compute(4, True)

    got("wu_p", w_at(um, v), dev_um)
    send(
        "wuf_p", wbuf.at[three, um, v, :, lower], wbuf.at[three, um, v, :, lower], dev_up
    )
    w_send(um, 1)
    got("wu_m", w_at(up, v), dev_up)
    send(
        "wuf_m", wbuf.at[three, up, v, :, upper], wbuf.at[three, up, v, :, upper], dev_um
    )
    w_send(up, 2)
    combine(0, True)
    combine(1, True)
    far_line(4)
    compute(5, False)
    compute(5, True)
    combine(2, True)
    combine(3, True)
    combine(4, False)
    combine(4, True)
    got("wuf_p", wbuf.at[three, u2, v, :, lower], dev_um)
    got("wuf_m", wbuf.at[three, u2, v, :, upper], dev_up)
    w_send(u2, 3)
    got("wv_p0", w_at(u, vm), dev_vm)
    send("wvf_p0", w_at(u, vm), w_at(u, vm), dev_vp)
    got("wv_p1", w_at(um, vm), dev_vm)
    send("wvf_p1", w_at(um, vm), w_at(um, vm), dev_vp)
    combine(5, False)
    got("wv_m0", w_at(u, vp), dev_vp)
    got("wv_m1", w_at(um, vp), dev_vp)
    got("wv_m2", w_at(up, vp), dev_vp)
    send("wvf_m2", w_at(up, vp), w_at(up, vp), dev_vm)
    combine(5, True)
    got("wv_m3", w_at(u2, vp), dev_vp)
    send("wvf_m3", w_at(u2, vp), w_at(u2, vp), dev_vm)
    got("wv_p2", w_at(up, vm), dev_vm)
    got("wv_p3", w_at(u2, vm), dev_vm)
    for k in range(6):
        finish(k, False)
        finish(k, True)
    for k in range(6):
        for cc in range(2):
            got(f"pt{k}{cc}", pt.at[1 - c, cc, span(k)], dev_mate)

    def rank(there, here):
        step = (2 * ((there + 4 - here) % 4)) % 5
        return step - step // 4

    with scope("assemble"):
        for src in range(2):
            own = c == src
            u_src, v_src = jnp.where(own, u, v), jnp.where(own, v, u)
            for vv in range(4):
                kv = rank(vv, v_src)
                for uu in range(4):
                    ku = rank(uu, u_src)
                    place = jnp.where(kv == 3, 12 + ku, 3 + 2 * ku + kv)
                    place = jnp.where(kv == 0, ku, place)
                    for zz in range(2):
                        xx, yy = (uu, vv) if src == 0 else (vv, uu)
                        first = SHARE * (xx * 16 + zz * 8 + yy * 2 + src)
                        row = PADDED * zz
                        for cc in range(2):
                            ptd[first : first + SHARE, half(cc)] = pt[
                                src, cc, place, row : row + SHARE, :
                            ]
        high = ptd[...].astype(BF16)
        ptd_h[...] = high
        ptd_l[...] = (ptd[...] - high.astype(F32)).astype(BF16)
        for q in range(3):
            pth[q] = high[q * WCOLS : (q + 1) * WCOLS, :]
        pth[3, :128] = jnp.zeros((128, 2 * BLOCK), BF16)
        pth[3, 128:] = high[3 * WCOLS :, :]

    for copy in own_w:
        copy.wait()
    for tag in range(4):
        if tag < 2:
            got(f"wvf_p{tag}", w_at(around[tag], v2), dev_vm)
        else:
            got(f"wvf_m{tag}", w_at(around[tag], v2), dev_vp)
    with scope("screen"):

        @pl.loop(0, 4)
        def _(rel):
            value = jnp.zeros((4 * WROWS, 2 * BLOCK), F32)
            for q in range(4):
                value += jnp.dot(
                    wbuf[rel, :, q].reshape(4 * WROWS, WCOLS),
                    pth[q],
                    preferred_element_type=F32,
                )
            rows = pl.ds(pl.multiple_of(rel * 4 * WROWS, 4 * WROWS), 4 * WROWS)
            high = value.astype(BF16)
            scr_h[rows, :] = high
            scr_l[rows, :] = (value - high.astype(F32)).astype(BF16)

    with scope("bs"):
        for slot in range(2):
            total = jnp.zeros((BLOCK, BLOCK), F32)
            for rel in range(4):
                base = ((h + rel) % 4) * 736 + c * 368
                for skip, first, count in ((0, 0, 288), (304, 288, 80)):
                    left_rows = pl.ds(rel * 4 * WROWS + skip, count)
                    right_rows = pl.ds(pl.multiple_of(base + first, 16), count)
                    for left, right in ((scr_h, ptd_h), (scr_h, ptd_l), (scr_l, ptd_h)):
                        total += lax.dot_general(
                            left[left_rows, half(slot)],
                            right[right_rows, half(slot)],
                            (((0,), (0,)), ((), ())),
                            preferred_element_type=F32,
                        )
            bs_own[slot] = total
    send("bs", bs_own, bs_mate, dev_mate)

    got("meta_mate", meta_all.at[1 - c], dev_mate)
    with scope("places"):
        item = lax.broadcasted_iota(jnp.int32, (NB_SIGMA // 2, BLOCK), 0)
        rows = (item // 64) * 128 + (item // 8) % 2 * 64 + (item // 16) % 4 * 16 + c * 8 + item % 8
        rows = rows.astype(F32)
        columns = lax.broadcasted_iota(jnp.int32, (NB_SIGMA, BLOCK), 0).astype(F32)
        places = []
        for cc in range(2):
            j = slot_of(0, cc)
            index = meta_all[cc, pl.ds(j, 1), :]
            weight = meta_all[cc, pl.ds(4 + j, 1), :]
            places.append(((rows == index).astype(BF16), (columns == index).astype(BF16), weight))
    got("bs", bs_mate, dev_mate)
    with scope("spread"):
        spread = jnp.zeros((NB_SIGMA // 2, NB_SIGMA), F32)
        for slot in range(2):
            to_rows, to_columns, weight = places[slot]
            block = (bs_own[slot] + bs_mate[slot]) * weight
            high = block.astype(BF16)
            low = (block - high.astype(F32)).astype(BF16)
            for term in (high, low):
                wide = lax.dot_general(
                    term, to_columns, (((1,), (1,)), ((), ())), preferred_element_type=F32
                )
                spread += jnp.dot(to_rows, wide.astype(BF16), preferred_element_type=F32)
        plane_s[...] = spread.astype(BF16).reshape(4, 4, 16, NB_SIGMA)
    for (dx, dy), (place, device) in plane.items():
        send(f"plane{dx}{dy}", plane_s.at[place[0], place[1]], plane_r.at[x, y], device)
    total = plane_s[x, y].astype(F32)
    for dx, dy in plane:
        source = (x + 4 - dx) % 4, (y + 4 - dy) % 4
        landed = plane_r.at[source[0], source[1]]
        got(f"plane{dx}{dy}", landed, plane[(4 - dx) % 4, (4 - dy) % 4][1])
        total += landed[...].astype(F32)
    for zz in range(2):
        for hh in range(4):
            first = 8 * zz + 2 * hh
            line_s[zz, hh] = total[first : first + 2, :]
    for (dz, dh), (place, device) in line.items():
        send(f"line{dz}{dh}", line_s.at[place[0], place[1]], line_r.at[zl, h], device)
    result = line_s[zl, h]
    for dz, dh in line:
        source = (zl + dz) % 2, (h + 4 - dh) % 4
        landed = line_r.at[source[0], source[1]]
        got(f"line{dz}{dh}", landed, line[dz, (4 - dh) % 4][1])
        result += landed[...]
    out_ref[...] = result
    for copy in sent:
        copy.wait_send()
    for name, device in pieces.items():
        remote(name, b_at(0, 0), b_at(0, 0), device).wait_send()
    for name, k, i, device in chunks_sent.values():
        piece = hop_s.at[i, span(k)]
        remote(name, piece, piece, device).wait_send()
    for core in range(2):

        @pl.when(c == core)
        def _():
            for name, device in sent_by_core[core]:
                whole = core == 0 or name in ("by_p", "by_m")
                piece = b_at(0, 0) if whole else b_half(0, 0, 0)
                remote(name, piece, piece, device).wait_send()

    assert len(ids) <= N_COPIES


def per_device(pair_density, eigvecs, screening, occupation, window_start, window_len, slot_band):
    block, plane_rows = pair_density.shape[1:]
    width = screening.shape[1]
    vmem = pl.BlockSpec(memory_space=pltpu.VMEM)
    hbm = pl.BlockSpec(memory_space=pltpu.HBM)
    scratch = [
        pltpu.VMEM((8, block, plane_rows), BF16),
        pltpu.VMEM((block, plane_rows), BF16),
        pltpu.VMEM((2, block // 2, plane_rows), BF16),
        pltpu.VMEM((block, plane_rows), BF16),
        pltpu.VMEM((SHARE, plane_rows), BF16),
        pltpu.VMEM((16, 2, PADDED, plane_rows), BF16),
        pltpu.VMEM((4, 4, 4, WROWS, WCOLS), BF16),
        pltpu.VMEM((4, 16, PIECE, 2 * block), F32),
    ]
    scratch += [pltpu.VMEM((2, 16, PIECE, block), BF16)] * 6
    scratch += [
        pltpu.VMEM((2, 2, 16, PIECE, block), F32),
        pltpu.VMEM((width, 2 * block), F32),
        pltpu.VMEM((4, WCOLS, 2 * block), BF16),
        pltpu.VMEM((width, 2 * block), BF16),
        pltpu.VMEM((width, 2 * block), BF16),
        pltpu.VMEM((16 * WROWS, 2 * block), BF16),
        pltpu.VMEM((16 * WROWS, 2 * block), BF16),
        pltpu.VMEM((2, 16, block), F32),
        pltpu.VMEM((2, 8, block), F32),
        pltpu.VMEM((2, block, block), F32),
        pltpu.VMEM((2, block, block), F32),
        pltpu.VMEM((4, 4, 16, NB_SIGMA), BF16),
        pltpu.VMEM((4, 4, 16, NB_SIGMA), BF16),
        pltpu.VMEM((2, 4, 2, NB_SIGMA), F32),
        pltpu.VMEM((2, 4, 2, NB_SIGMA), F32),
        pltpu.SemaphoreType.DMA((N_COPIES,)),
        pltpu.SemaphoreType.DMA((N_COPIES,)),
        pltpu.SemaphoreType.DMA((24,)),
    ]
    smem = pl.BlockSpec(memory_space=pltpu.SMEM)
    return pl.pallas_call(
        main_kernel,
        out_shape=jax.ShapeDtypeStruct((2, NB_SIGMA), F32),
        in_specs=[smem, smem, smem, vmem, hbm, hbm, hbm],
        out_specs=vmem,
        scratch_shapes=scratch,
        compiler_params=pltpu.CompilerParams(
            collective_id=0, has_side_effects=True, vmem_limit_bytes=60 * 1024 * 1024
        ),
        name="cohsex",
    )(
        window_start,
        window_len,
        slot_band,
        occupation.reshape(1, -1),
        pair_density,
        eigvecs,
        screening,
    )


def solution(mesh):
    return jax.shard_map(
        per_device,
        mesh=mesh,
        in_specs=(
            P("band", None, "pw"),
            P("band", "pw"),
            P("pw", None),
            P(),
            P("band"),
            P("band"),
            P("band"),
        ),
        out_specs=P(("band", "pw"), None),
        check_vma=False,
    )
```

```python
import jax
import jax.numpy as jnp
from jax import lax
from jax.experimental import pallas as pl
from jax.experimental.pallas import tpu as pltpu
from jax.sharding import PartitionSpec as P

NB_SIGMA = 512
BLOCK = 128
F32 = jnp.float32
BF16 = jnp.bfloat16
HIGHEST = lax.Precision.HIGHEST
SHARE, PADDED = 46, 48
PIECE = 2 * PADDED
CHUNKS = ((0, 4), (4, 6), (6, 8), (8, 10), (10, 12), (12, 16))


def place_of(kv, ku):
    if kv == 0:
        return ku
    return 12 + ku if kv == 3 else 3 + 2 * ku + kv


WROWS, WCOLS = 96, 768
N_COPIES = 280
scope = jax.named_scope


def main_kernel(
    start_ref,
    len_ref,
    slot_ref,
    occ_ref,
    a_ref,
    eig_ref,
    w_ref,
    out_ref,
    a_all,
    spare,
    relay,
    own3,
    share,
    bbuf,
    wbuf,
    part,
    hop_s,
    hop_r,
    dir_s,
    dir_r,
    comb_s,
    comb_r,
    pt,
    ptd,
    pth,
    ptd_h,
    ptd_l,
    scr,
    scr_h,
    scr_l,
    meta_buf,
    meta_all,
    bs_own,
    bs_mate,
    plane_s,
    plane_r,
    line_s,
    line_r,
    ssem,
    rsem,
    lsem,
):
    band = lax.axis_index("band")
    h = lax.axis_index("pw")
    x = band // 16
    zl = (band // 8) % 2
    y = (band // 2) % 4
    c = band % 2
    u = x * (1 - c) + y * c
    v = y * (1 - c) + x * c
    su = 16 - 14 * c
    sv = 2 + 14 * c
    hp, hm, h2 = (h + 1) % 4, (h + 3) % 4, (h + 2) % 4
    up, um, u2 = (u + 1) % 4, (u + 3) % 4, (u + 2) % 4
    vp, vm, v2 = (v + 1) % 4, (v + 3) % 4, (v + 2) % 4

    def at_uv(uu, vv):
        return (uu * su + vv * sv + zl * 8 + c, h)

    dev_up, dev_um = at_uv(up, v), at_uv(um, v)
    dev_vp, dev_vm = at_uv(u, vp), at_uv(u, vm)
    dev_hp, dev_hm = (band, hp), (band, hm)
    dev_zl = (x * 16 + (1 - zl) * 8 + y * 2 + c, h)
    dev_mate = (x * 16 + zl * 8 + y * 2 + 1 - c, h)
    dev_far = (((x + 2) % 4) * 16 + zl * 8 + y * 2 + c, h)

    barrier = pltpu.get_barrier_semaphore()
    plane = {}
    for dx in range(4):
        for dy in range(4):
            if dx or dy:
                place = ((x + dx) % 4, (y + dy) % 4)
                plane[dx, dy] = place, (place[0] * 16 + zl * 8 + place[1] * 2 + c, h)
    line = {}
    for dz in range(2):
        for dh in range(4):
            if dz or dh:
                place = ((zl + dz) % 2, (h + dh) % 4)
                line[dz, dh] = place, (x * 16 + place[0] * 8 + y * 2 + c, place[1])
    dev_xp, dev_xm = plane[1, 0][1], plane[3, 0][1]
    peers = [dev_mate, dev_up, dev_um, dev_vp, dev_vm, dev_hp, dev_hm, dev_zl, dev_far]
    for peer in peers:
        pl.semaphore_signal(barrier, inc=1, device_id=peer, device_id_type=pl.DeviceIdType.MESH)

    own_b = pltpu.make_async_copy(eig_ref, share, lsem.at[23])
    own_b.start()
    lane = lax.broadcasted_iota(jnp.int32, (1, BLOCK), 1)
    for j in range(5):
        kept = (lane < len_ref[j]) & (slot_ref[j] >= 0)
        meta_buf[0, j : j + 1, :] = jnp.where(kept, start_ref[j] + lane, -1).astype(F32)
        value = jnp.sum(jnp.where(lane == slot_ref[j], occ_ref[...], 0.0), axis=1, keepdims=True)
        meta_buf[0, 8 + j : 9 + j, :] = jnp.broadcast_to(0.5 - value, (1, BLOCK))
    taking = slot_ref[3] < 0
    meta_buf[0, 5:6, :] = jnp.where(taking, 1.0, 0.0) + jnp.zeros((1, BLOCK), F32)
    for rel in range(1, 4):
        for p in range(4):
            wbuf[rel, p, 3, :, :128] = jnp.zeros((WROWS, 128), BF16)
    own_b.wait()
    bbuf[0, zl, :SHARE] = share[...]
    bbuf[0, zl, SHARE:] = jnp.zeros((PADDED - SHARE, share.shape[1]), BF16)
    with scope('barrier'):
        pl.semaphore_wait(barrier, len(peers))

    ids = {}
    sent = []
    sent_by_core = ([], [])
    pieces = {}

    def remote(name, src, dst, device):
        i = ids.setdefault(name, len(ids))
        return pltpu.make_async_remote_copy(
            src_ref=src,
            dst_ref=dst,
            send_sem=ssem.at[i],
            recv_sem=rsem.at[i],
            device_id=device,
            device_id_type=pl.DeviceIdType.MESH,
        )

    def send(name, src, dst, device, into=sent):
        copy = remote(name, src, dst, device)
        copy.start()
        into.append(copy if into is sent else (name, device))

    def got(name, landing, device):
        with scope("got_" + name):
            remote(name, landing, landing, device).wait_recv()

    local_ids = {}

    def local(name, src, dst):
        i = local_ids.setdefault(name, len(local_ids))
        copy = pltpu.make_async_copy(src, dst, lsem.at[i])
        copy.start()
        return copy

    oz = 1 - zl
    around = (u, um, up, u2)
    order = (v, vm, vp, v2)

    def b_half(kv, ku, zz):
        return bbuf.at[place_of(kv, ku), zz]

    def b_at(kv, ku):
        return bbuf.at[place_of(kv, ku)]

    kinds = {"full": (128, 640), "lower": (128, 256), "upper": (384, 384)}

    def w_copies(kind, p, q):
        lanes = kinds[kind]
        yield "a", (16, WROWS - 16), lanes, None
        yield "b", (0, 16), lanes, p != 3
        if kind != "upper":
            yield "c", (0, WROWS), (0, 128), q != 3

    def guarded(needed, run):
        if needed is None:
            run()
        else:
            pl.when(needed)(run)

    def w_own(p, q):
        def view(rows, lanes):
            row = pl.multiple_of(c * 368 + p * WROWS - 16 * (p // 3) + rows[0], 16)
            col = pl.multiple_of(q * WCOLS - 128 * (q // 3) + lanes[0], 128)
            return w_ref.at[pl.ds(row, rows[1]), pl.ds(col, lanes[1])]

        return view

    def w_one(rel):
        return lambda rows, lanes: wbuf.at[rel, u, v, pl.ds(*rows), pl.ds(*lanes)]

    def w_at(uu, vv):
        return lambda rows, lanes: wbuf.at[pl.ds(1, 3), uu, vv, pl.ds(*rows), pl.ds(*lanes)]

    w_sent = []

    def w_move(name, src, dst, device, p, q, kind="full"):
        for tag, rows, lanes, needed in w_copies(kind, p, q):
            guarded(
                needed,
                lambda: remote(name + tag, src(rows, lanes), dst(rows, lanes), device).start(),
            )
        w_sent.append((name, src, device, p, q, kind))

    def w_got(name, landing, device, p, q, kind="full"):
        with scope("got_" + name):
            for tag, rows, lanes, needed in w_copies(kind, p, q):

                def run():
                    here = landing(rows, lanes)
                    remote(name + tag, here, here, device).wait_recv()

                guarded(needed, run)

    def w_left(name, src, device, p, q, kind):
        for tag, rows, lanes, needed in w_copies(kind, p, q):

            def run():
                here = src(rows, lanes)
                remote(name + tag, here, here, device).wait_send()

            guarded(needed, run)

    def w_send(uu, tag):
        w_move(f"wv_p{tag}", w_at(uu, v), w_at(uu, v), dev_vp, uu, v)
        w_move(f"wv_m{tag}", w_at(uu, v), w_at(uu, v), dev_vm, uu, v)

    def b_send(ku):
        for name, kv, device in ((f"bv_p{ku}", 1, dev_vp), (f"bv_m{ku}", 2, dev_vm)):
            remote(name, b_at(0, ku), b_at(kv, ku), device).start()
            pieces[name] = device

    def b_got(kv, ku):
        if ku:
            got(f"bv_{'pm'[kv - 1]}{ku}", b_at(kv, ku), dev_vm if kv == 1 else dev_vp)
        else:
            for zz, tag in ((zl, "a"), (oz, "b")):
                device = dev_vm if kv == 1 else dev_vp
                got(f"bv_{'pm'[kv - 1]}0{tag}", b_half(kv, 0, zz), device)

    def far_line(step, core=None):
        def core0():
            for kv, ku in (((1, 0),), ((1, 1),), ((2, 2),), ((2, 3),), ())[step]:
                device = dev_vp if kv == 1 else dev_vm
                send(f"bf{kv}{ku}", b_at(kv, ku), b_at(3, ku), device, sent_by_core[0])
            if step == 4:
                for ku in range(4):
                    got(f"bf{1 if ku < 2 else 2}{ku}", b_at(3, ku), dev_vm if ku < 2 else dev_vp)

        def core1():
            into = sent_by_core[1]
            if step == 0:
                send("bx_p", b_half(1, 0, zl), b_half(3, 0, zl), dev_vp, into)
                send("bx_m", b_half(2, 0, oz), b_half(3, 0, oz), dev_vm, into)
            elif step == 1:
                pass
            elif step == 2:
                got("bx_p", b_half(3, 0, zl), dev_vm)
                got("bx_m", b_half(3, 0, oz), dev_vp)
                send("by_p", b_at(3, 0), b_at(3, 1), dev_up, into)
                send("by_m", b_at(3, 0), b_at(3, 2), dev_um, into)
            elif step == 3:
                got("by_p", b_at(3, 1), dev_um)
                send("byf_p", b_half(3, 1, zl), b_half(3, 3, zl), dev_up, into)
                got("by_m", b_at(3, 2), dev_up)
                send("byf_m", b_half(3, 2, oz), b_half(3, 3, oz), dev_um, into)
            else:
                got("byf_p", b_half(3, 3, zl), dev_um)
                got("byf_m", b_half(3, 3, oz), dev_up)

        if core != 1:
            pl.when(c == 0)(core0)
        if core != 0:
            pl.when(c == 1)(core1)

    send("zl", b_half(0, 0, zl), b_half(0, 0, zl), dev_zl)
    send("bu_p0", b_half(0, 0, zl), b_half(0, 1, zl), dev_up)
    send("bu_m0", b_half(0, 0, zl), b_half(0, 2, zl), dev_um)
    send("meta_far", meta_buf.at[0], meta_buf.at[1], dev_far)
    own_a = []
    for j in range(3):
        own_a.append(local(f"a{j}", a_ref.at[j], a_all.at[2 * j + c]))
        send(f"mate_a{j}", a_ref.at[j], a_all.at[2 * j + c], dev_mate)
    own_a.append(local("a3", a_ref.at[3], own3))
    send("bv_p0a", b_half(0, 0, zl), b_half(1, 0, zl), dev_vp)
    send("bv_m0a", b_half(0, 0, zl), b_half(2, 0, zl), dev_vm)

    got("zl", b_half(0, 0, oz), dev_zl)
    send("bu_p1", b_half(0, 0, oz), b_half(0, 1, oz), dev_up)
    send("bu_m1", b_half(0, 0, oz), b_half(0, 2, oz), dev_um)
    send("bv_p0b", b_half(0, 0, oz), b_half(1, 0, oz), dev_vp)
    send("bv_m0b", b_half(0, 0, oz), b_half(2, 0, oz), dev_vm)
    w_move("wz_m", w_own(u, v), w_one(1), dev_hm, u, v)
    w_move("wz_p", w_own(u, v), w_one(3), dev_hp, u, v)

    got("bu_p0", b_half(0, 1, zl), dev_um)
    send("buf_p", b_half(0, 1, zl), b_half(0, 3, zl), dev_up)
    got("bu_m0", b_half(0, 2, zl), dev_up)
    got("bu_m1", b_half(0, 2, oz), dev_up)
    send("buf_m", b_half(0, 2, oz), b_half(0, 3, oz), dev_um)
    near, far = pl.ds(0, BLOCK // 2), pl.ds(BLOCK // 2, BLOCK // 2)
    send("spare_p", a_ref.at[4, near], relay.at[0], dev_xp)
    send("spare_m", a_ref.at[4, far], relay.at[1], dev_xm)
    got("bu_p1", b_half(0, 1, oz), dev_um)
    b_send(1)
    pl.when(c == 0)(lambda: b_send(2))
    w_got("wz_m", w_one(1), dev_hp, u, v)
    w_move("wzf_m", w_one(1), w_one(2), dev_hm, u, v, "lower")
    w_got("wz_p", w_one(3), dev_hm, u, v)
    w_move("wzf_p", w_one(3), w_one(2), dev_hp, u, v, "upper")
    for j in range(3):
        own_a[j].wait()
        got(f"mate_a{j}", a_all.at[2 * j + 1 - c], dev_mate)
    got("buf_p", b_half(0, 3, zl), dev_um)
    got("buf_m", b_half(0, 3, oz), dev_up)

    def slot_of(r, cc):
        return (h + r + 7 - 2 * cc - zl) % 4

    def half(cc):
        return pl.ds(cc * BLOCK, BLOCK)

    def project(k, j):
        lo, hi = CHUNKS[k]
        rows = (hi - lo) * PIECE
        part[j, lo:hi] = lax.dot_general(
            bbuf[lo:hi].reshape(rows, bbuf.shape[-1]),
            a_all[pl.ds(2 * j, 2)].reshape(2 * BLOCK, bbuf.shape[-1]),
            (((1,), (1,)), ((), ())),
            preferred_element_type=F32,
        ).reshape(hi - lo, PIECE, 2 * BLOCK)

    def span(k):
        return pl.ds(CHUNKS[k][0], CHUNKS[k][1] - CHUNKS[k][0])

    chunks_sent = {}

    def phase(late, j, run):
        pl.when((j == 3) if late else (j != 3))(run)

    def compute(k, late):
        with scope(f"compute{k}_{late}"):
            if late:
                project(k, 3)
            else:

                @pl.loop(0, 3)
                def _(j):
                    project(k, j)

            for name, i, r, cc, send_buf, recv_buf, device in (
                ("hop", 0, 2, 0, hop_s, hop_r, dev_hm),
                ("hop", 1, 2, 1, hop_s, hop_r, dev_hp),
                ("dir", 0, 3, 1, dir_s, dir_r, dev_hm),
                ("dir", 1, 1, 0, dir_s, dir_r, dev_hp),
            ):
                j = slot_of(r, cc)
                copy = remote(
                    f"{name}{k}{i}", send_buf.at[i, span(k)], recv_buf.at[i, span(k)], device
                )
                chunks_sent[f"{name}{k}{i}"] = (f"{name}{k}{i}", k, i, device)

                def run():
                    send_buf[i, span(k)] = part[j, span(k), :, half(cc)].astype(BF16)
                    copy.start()

                phase(late, j, run)

    def combine(k, late, core=None):
        for i, r, cc, source, device in ((0, 3, 0, dev_hp, dev_hm), (1, 1, 1, dev_hm, dev_hp)):
            j = slot_of(r, cc)
            copy = remote(
                f"comb{k}{i}", comb_s.at[i, span(k)], comb_r.at[i, span(k)], device
            )
            chunks_sent[f"comb{k}{i}"] = (f"comb{k}{i}", k, i, device)

            def run():
                got(f"hop{k}{i}", hop_r.at[i, span(k)], source)
                total = part[j, span(k), :, half(cc)] + hop_r[i, span(k)].astype(F32)
                comb_s[i, span(k)] = total.astype(BF16)
                copy.start()

            if core is None:
                phase(late, j, run)
            else:
                pl.when((j != 3) & (c == core))(run)

    def finish(k, late):
        for cc, first, second in ((0, dev_hp, dev_hm), (1, dev_hm, dev_hp)):
            j = slot_of(0, cc)
            mine = pt.at[c, cc, span(k)]
            to_mate = remote(f"pt{k}{cc}", mine, mine, dev_mate)
            if not late:
                sent.append(to_mate)

            def run():
                got(f"dir{k}{1 - cc}", dir_r.at[1 - cc, span(k)], second)
                got(f"comb{k}{cc}", comb_r.at[cc, span(k)], first)
                pt[c, cc, span(k)] = part[j, span(k), :, half(cc)] + (
                    comb_r[cc, span(k)].astype(F32) + dir_r[1 - cc, span(k)].astype(F32)
                )
                to_mate.start()

            phase(late, j, run)

    compute(0, False)

    got("meta_far", meta_buf.at[1], dev_far)
    swap = meta_buf[0, 5:6, :] > 0.5
    for row, far_row in ((0, 4), (8, 12)):
        first = row // 2
        meta_all[c, first : first + 3, :] = meta_buf[0, row : row + 3, :]
        meta_all[c, first + 3 : first + 4, :] = jnp.where(
            swap, meta_buf[1, far_row : far_row + 1, :], meta_buf[0, row + 3 : row + 4, :]
        )
    send("meta_mate", meta_all.at[c], meta_all.at[c], dev_mate)

    b_got(1, 0)
    b_got(2, 0)
    far_line(0)
    compute(1, False)
    got("spare_p", relay.at[0], dev_xm)
    send("spare_pf", relay.at[0], spare.at[near], dev_xp)
    got("spare_m", relay.at[1], dev_xp)
    send("spare_mf", relay.at[1], spare.at[far], dev_xm)
    pl.when(c == 1)(lambda: b_send(2))
    b_send(3)
    combine(0, False, 1)
    b_got(1, 1)
    far_line(1)
    b_got(2, 1)
    compute(2, False)
    combine(0, False, 0)
    far_line(2, 1)

    def fourth():
        b_got(2, 2)
        b_got(1, 2)
        compute(3, False)

    def fifth(core):
        b_got(2, 3)
        if core == 0:
            far_line(3, 0)
        b_got(1, 3)
        compute(4, False)

    @pl.when(c == 0)
    def _():
        b_got(2, 2)
        far_line(2, 0)
        b_got(1, 2)
        compute(3, False)
        combine(1, False, 0)

    got("spare_pf", spare.at[near], dev_xm)
    got("spare_mf", spare.at[far], dev_xp)
    own_a[3].wait()
    a_all[6 + c] = jnp.where(taking, spare[...], own3[...])
    send("mate_a3", a_all.at[6 + c], a_all.at[6 + c], dev_mate)

    @pl.when(c == 0)
    def _():
        fifth(0)
        combine(2, False, 0)

    combine(1, False, 1)
    got("mate_a3", a_all.at[7 - c], dev_mate)
    for k in range(3):
        compute(k, True)

    w_got("wzf_m", w_one(2), dev_hp, u, v, "lower")
    w_got("wzf_p", w_one(2), dev_hm, u, v, "upper")
    w_move("wu_p", w_at(u, v), w_at(u, v), dev_up, u, v)
    w_move("wu_m", w_at(u, v), w_at(u, v), dev_um, u, v)
    own_w = []
    for p in range(4):
        for q in range(4):
            own_w.append(local(f"w{p}{q}", w_own(p, q)((0, WROWS), (0, WCOLS)), wbuf.at[0, p, q]))
    combine(2, False, 1)

    @pl.when(c == 1)
    def _():
        fourth()
        far_line(3, 1)
        fifth(1)

    compute(3, True)
    w_send(u, 0)
    compute(4, True)

    w_got("wu_p", w_at(um, v), dev_um, um, v)
    w_move("wuf_p", w_at(um, v), w_at(um, v), dev_up, um, v, "lower")
    w_send(um, 1)
    w_got("wu_m", w_at(up, v), dev_up, up, v)
    w_move("wuf_m", w_at(up, v), w_at(up, v), dev_um, up, v, "upper")
    w_send(up, 2)
    combine(3, False)
    combine(0, True)
    combine(1, True)
    far_line(4)
    compute(5, False)
    compute(5, True)
    combine(2, True)
    combine(3, True)
    combine(4, False)
    combine(4, True)
    w_got("wuf_p", w_at(u2, v), dev_um, u2, v, "lower")
    w_got("wuf_m", w_at(u2, v), dev_up, u2, v, "upper")
    w_send(u2, 3)
    w_got("wv_p0", w_at(u, vm), dev_vm, u, vm)
    w_move("wvf_p0", w_at(u, vm), w_at(u, vm), dev_vp, u, vm)
    w_got("wv_p1", w_at(um, vm), dev_vm, um, vm)
    w_move("wvf_p1", w_at(um, vm), w_at(um, vm), dev_vp, um, vm)
    combine(5, False)
    w_got("wv_m0", w_at(u, vp), dev_vp, u, vp)
    w_got("wv_m1", w_at(um, vp), dev_vp, um, vp)
    w_got("wv_m2", w_at(up, vp), dev_vp, up, vp)
    w_move("wvf_m2", w_at(up, vp), w_at(up, vp), dev_vm, up, vp)
    combine(5, True)
    w_got("wv_m3", w_at(u2, vp), dev_vp, u2, vp)
    w_move("wvf_m3", w_at(u2, vp), w_at(u2, vp), dev_vm, u2, vp)
    w_got("wv_p2", w_at(up, vm), dev_vm, up, vm)
    w_got("wv_p3", w_at(u2, vm), dev_vm, u2, vm)
    for k in range(6):
        finish(k, False)
        finish(k, True)
    for k in range(6):
        for cc in range(2):
            got(f"pt{k}{cc}", pt.at[1 - c, cc, span(k)], dev_mate)

    def rank(there, here):
        step = (2 * ((there + 4 - here) % 4)) % 5
        return step - step // 4

    with scope("assemble"):
        for src in range(2):
            own = c == src
            u_src, v_src = jnp.where(own, u, v), jnp.where(own, v, u)
            for vv in range(4):
                kv = rank(vv, v_src)
                for uu in range(4):
                    ku = rank(uu, u_src)
                    place = jnp.where(kv == 3, 12 + ku, 3 + 2 * ku + kv)
                    place = jnp.where(kv == 0, ku, place)
                    for zz in range(2):
                        xx, yy = (uu, vv) if src == 0 else (vv, uu)
                        first = SHARE * (xx * 16 + zz * 8 + yy * 2 + src)
                        row = PADDED * zz
                        for cc in range(2):
                            ptd[first : first + SHARE, half(cc)] = pt[
                                src, cc, place, row : row + SHARE, :
                            ]
        high = ptd[...].astype(BF16)
        ptd_h[...] = high
        ptd_l[...] = (ptd[...] - high.astype(F32)).astype(BF16)
        for q in range(3):
            pth[q] = high[q * WCOLS : (q + 1) * WCOLS, :]
        pth[3, :128] = jnp.zeros((128, 2 * BLOCK), BF16)
        pth[3, 128:] = high[3 * WCOLS :, :]

    for copy in own_w:
        copy.wait()

    def screened(rel, q):
        return jnp.dot(
            wbuf[rel, :, q].reshape(4 * WROWS, WCOLS), pth[q], preferred_element_type=F32
        )

    def rows_of(rel):
        return pl.ds(pl.multiple_of(rel * 4 * WROWS, 4 * WROWS), 4 * WROWS)

    with scope("screen"):

        @pl.loop(0, 4)
        def _(rel):
            scr[rows_of(rel), :] = screened(rel, v) + screened(rel, vm) + screened(rel, vp)

    for tag in range(4):
        if tag < 2:
            w_got(f"wvf_p{tag}", w_at(around[tag], v2), dev_vm, around[tag], v2)
        else:
            w_got(f"wvf_m{tag}", w_at(around[tag], v2), dev_vp, around[tag], v2)
    with scope("screen_last"):

        @pl.loop(0, 4)
        def _(rel):
            value = scr[rows_of(rel), :] + screened(rel, v2)
            high = value.astype(BF16)
            scr_h[rows_of(rel), :] = high
            scr_l[rows_of(rel), :] = (value - high.astype(F32)).astype(BF16)

    with scope("bs"):
        for slot in range(2):
            total = jnp.zeros((BLOCK, BLOCK), F32)
            for rel in range(4):
                base = ((h + rel) % 4) * 736 + c * 368
                for skip, first, count in ((0, 0, 288), (304, 288, 80)):
                    left_rows = pl.ds(rel * 4 * WROWS + skip, count)
                    right_rows = pl.ds(pl.multiple_of(base + first, 16), count)
                    for left, right in ((scr_h, ptd_h), (scr_h, ptd_l), (scr_l, ptd_h)):
                        total += lax.dot_general(
                            left[left_rows, half(slot)],
                            right[right_rows, half(slot)],
                            (((0,), (0,)), ((), ())),
                            preferred_element_type=F32,
                        )
            bs_own[slot] = total
    send("bs", bs_own, bs_mate, dev_mate)

    got("meta_mate", meta_all.at[1 - c], dev_mate)
    with scope("places"):
        item = lax.broadcasted_iota(jnp.int32, (NB_SIGMA // 2, BLOCK), 0)
        rows = (item // 64) * 128 + (item // 8) % 2 * 64 + (item // 16) % 4 * 16 + c * 8 + item % 8
        rows = rows.astype(F32)
        columns = lax.broadcasted_iota(jnp.int32, (NB_SIGMA, BLOCK), 0).astype(F32)
        places = []
        for cc in range(2):
            j = slot_of(0, cc)
            index = meta_all[cc, pl.ds(j, 1), :]
            weight = meta_all[cc, pl.ds(4 + j, 1), :]
            places.append(((rows == index).astype(BF16), (columns == index).astype(BF16), weight))
    got("bs", bs_mate, dev_mate)
    with scope("spread"):
        spread = jnp.zeros((NB_SIGMA // 2, NB_SIGMA), F32)
        for slot in range(2):
            to_rows, to_columns, weight = places[slot]
            block = (bs_own[slot] + bs_mate[slot]) * weight
            high = block.astype(BF16)
            low = (block - high.astype(F32)).astype(BF16)
            for term in (high, low):
                wide = lax.dot_general(
                    term, to_columns, (((1,), (1,)), ((), ())), preferred_element_type=F32
                )
                spread += jnp.dot(to_rows, wide.astype(BF16), preferred_element_type=F32)
        plane_s[...] = spread.astype(BF16).reshape(4, 4, 16, NB_SIGMA)
    for (dx, dy), (place, device) in plane.items():
        send(f"plane{dx}{dy}", plane_s.at[place[0], place[1]], plane_r.at[x, y], device)
    total = plane_s[x, y].astype(F32)
    for dx, dy in plane:
        source = (x + 4 - dx) % 4, (y + 4 - dy) % 4
        landed = plane_r.at[source[0], source[1]]
        got(f"plane{dx}{dy}", landed, plane[(4 - dx) % 4, (4 - dy) % 4][1])
        total += landed[...].astype(F32)
    for zz in range(2):
        for hh in range(4):
            first = 8 * zz + 2 * hh
            line_s[zz, hh] = total[first : first + 2, :]
    for (dz, dh), (place, device) in line.items():
        send(f"line{dz}{dh}", line_s.at[place[0], place[1]], line_r.at[zl, h], device)
    result = line_s[zl, h]
    for dz, dh in line:
        source = (zl + dz) % 2, (h + 4 - dh) % 4
        landed = line_r.at[source[0], source[1]]
        got(f"line{dz}{dh}", landed, line[dz, (4 - dh) % 4][1])
        result += landed[...]
    out_ref[...] = result
    for copy in sent:
        copy.wait_send()
    for item in w_sent:
        w_left(*item)
    for name, device in pieces.items():
        remote(name, b_at(0, 0), b_at(0, 0), device).wait_send()
    for name, k, i, device in chunks_sent.values():
        piece = hop_s.at[i, span(k)]
        remote(name, piece, piece, device).wait_send()
    for core in range(2):

        @pl.when(c == core)
        def _():
            for name, device in sent_by_core[core]:
                whole = core == 0 or name in ("by_p", "by_m")
                piece = b_at(0, 0) if whole else b_half(0, 0, 0)
                remote(name, piece, piece, device).wait_send()

    assert len(ids) <= N_COPIES


def per_device(pair_density, eigvecs, screening, occupation, window_start, window_len, slot_band):
    block, plane_rows = pair_density.shape[1:]
    width = screening.shape[1]
    vmem = pl.BlockSpec(memory_space=pltpu.VMEM)
    hbm = pl.BlockSpec(memory_space=pltpu.HBM)
    scratch = [
        pltpu.VMEM((8, block, plane_rows), BF16),
        pltpu.VMEM((block, plane_rows), BF16),
        pltpu.VMEM((2, block // 2, plane_rows), BF16),
        pltpu.VMEM((block, plane_rows), BF16),
        pltpu.VMEM((SHARE, plane_rows), BF16),
        pltpu.VMEM((16, 2, PADDED, plane_rows), BF16),
        pltpu.VMEM((4, 4, 4, WROWS, WCOLS), BF16),
        pltpu.VMEM((4, 16, PIECE, 2 * block), F32),
    ]
    scratch += [pltpu.VMEM((2, 16, PIECE, block), BF16)] * 6
    scratch += [
        pltpu.VMEM((2, 2, 16, PIECE, block), F32),
        pltpu.VMEM((width, 2 * block), F32),
        pltpu.VMEM((4, WCOLS, 2 * block), BF16),
        pltpu.VMEM((width, 2 * block), BF16),
        pltpu.VMEM((width, 2 * block), BF16),
        pltpu.VMEM((16 * WROWS, 2 * block), F32),
        pltpu.VMEM((16 * WROWS, 2 * block), BF16),
        pltpu.VMEM((16 * WROWS, 2 * block), BF16),
        pltpu.VMEM((2, 16, block), F32),
        pltpu.VMEM((2, 8, block), F32),
        pltpu.VMEM((2, block, block), F32),
        pltpu.VMEM((2, block, block), F32),
        pltpu.VMEM((4, 4, 16, NB_SIGMA), BF16),
        pltpu.VMEM((4, 4, 16, NB_SIGMA), BF16),
        pltpu.VMEM((2, 4, 2, NB_SIGMA), F32),
        pltpu.VMEM((2, 4, 2, NB_SIGMA), F32),
        pltpu.SemaphoreType.DMA((N_COPIES,)),
        pltpu.SemaphoreType.DMA((N_COPIES,)),
        pltpu.SemaphoreType.DMA((24,)),
    ]
    smem = pl.BlockSpec(memory_space=pltpu.SMEM)
    return pl.pallas_call(
        main_kernel,
        out_shape=jax.ShapeDtypeStruct((2, NB_SIGMA), F32),
        in_specs=[smem, smem, smem, vmem, hbm, hbm, hbm],
        out_specs=vmem,
        scratch_shapes=scratch,
        compiler_params=pltpu.CompilerParams(
            collective_id=0, has_side_effects=True, vmem_limit_bytes=60 * 1024 * 1024
        ),
        name="cohsex",
    )(
        window_start,
        window_len,
        slot_band,
        occupation.reshape(1, -1),
        pair_density,
        eigvecs,
        screening,
    )


def solution(mesh):
    return jax.shard_map(
        per_device,
        mesh=mesh,
        in_specs=(
            P("band", None, "pw"),
            P("band", "pw"),
            P("pw", None),
            P(),
            P("band"),
            P("band"),
            P("band"),
        ),
        out_specs=P(("band", "pw"), None),
        check_vma=False,
    )
```

```python
import jax
import jax.numpy as jnp
from jax import lax
from jax.experimental import pallas as pl
from jax.experimental.pallas import tpu as pltpu
from jax.sharding import PartitionSpec as P

NB_SIGMA = 512
BLOCK = 128
F32 = jnp.float32
BF16 = jnp.bfloat16
HIGHEST = lax.Precision.HIGHEST
SHARE, PADDED = 46, 48
PIECE = 2 * PADDED
CHUNKS = ((0, 4), (4, 6), (6, 8), (8, 10), (10, 12), (12, 16))


def place_of(kv, ku):
    if kv == 0:
        return ku
    return 12 + ku if kv == 3 else 3 + 2 * ku + kv


WROWS, WCOLS = 96, 768
N_COPIES = 166
scope = jax.named_scope


def main_kernel(
    start_ref,
    len_ref,
    slot_ref,
    occ_ref,
    a_ref,
    eig_ref,
    w_ref,
    out_ref,
    a_all,
    spare,
    relay,
    own3,
    share,
    bbuf,
    wbuf,
    part,
    hop_s,
    hop_r,
    dir_s,
    dir_r,
    comb_s,
    comb_r,
    pt,
    ptd,
    pth,
    ptd_h,
    ptd_l,
    scr,
    scr_h,
    scr_l,
    meta_buf,
    meta_all,
    bs_own,
    bs_mate,
    plane_s,
    plane_r,
    line_s,
    line_r,
    ssem,
    rsem,
    lsem,
):
    band = lax.axis_index("band")
    h = lax.axis_index("pw")
    x = band // 16
    zl = (band // 8) % 2
    y = (band // 2) % 4
    c = band % 2
    u = x * (1 - c) + y * c
    v = y * (1 - c) + x * c
    su = 16 - 14 * c
    sv = 2 + 14 * c
    hp, hm, h2 = (h + 1) % 4, (h + 3) % 4, (h + 2) % 4
    up, um, u2 = (u + 1) % 4, (u + 3) % 4, (u + 2) % 4
    vp, vm, v2 = (v + 1) % 4, (v + 3) % 4, (v + 2) % 4

    def at_uv(uu, vv):
        return (uu * su + vv * sv + zl * 8 + c, h)

    dev_up, dev_um = at_uv(up, v), at_uv(um, v)
    dev_vp, dev_vm = at_uv(u, vp), at_uv(u, vm)
    dev_hp, dev_hm = (band, hp), (band, hm)
    dev_zl = (x * 16 + (1 - zl) * 8 + y * 2 + c, h)
    dev_mate = (x * 16 + zl * 8 + y * 2 + 1 - c, h)
    dev_far = (((x + 2) % 4) * 16 + zl * 8 + y * 2 + c, h)

    barrier = pltpu.get_barrier_semaphore()
    plane = {}
    for dx in range(4):
        for dy in range(4):
            if dx or dy:
                place = ((x + dx) % 4, (y + dy) % 4)
                plane[dx, dy] = place, (place[0] * 16 + zl * 8 + place[1] * 2 + c, h)
    line = {}
    for dz in range(2):
        for dh in range(4):
            if dz or dh:
                place = ((zl + dz) % 2, (h + dh) % 4)
                line[dz, dh] = place, (x * 16 + place[0] * 8 + y * 2 + c, place[1])
    dev_xp, dev_xm = plane[1, 0][1], plane[3, 0][1]
    peers = [dev_mate, dev_up, dev_um, dev_vp, dev_vm, dev_hp, dev_hm, dev_zl, dev_far]
    for peer in peers:
        pl.semaphore_signal(barrier, inc=1, device_id=peer, device_id_type=pl.DeviceIdType.MESH)

    own_b = pltpu.make_async_copy(eig_ref, share, lsem.at[20])
    own_b.start()
    lane = lax.broadcasted_iota(jnp.int32, (1, BLOCK), 1)
    for j in range(5):
        kept = (lane < len_ref[j]) & (slot_ref[j] >= 0)
        meta_buf[0, j : j + 1, :] = jnp.where(kept, start_ref[j] + lane, -1).astype(F32)
        value = jnp.sum(jnp.where(lane == slot_ref[j], occ_ref[...], 0.0), axis=1, keepdims=True)
        meta_buf[0, 8 + j : 9 + j, :] = jnp.broadcast_to(0.5 - value, (1, BLOCK))
    taking = slot_ref[3] < 0
    meta_buf[0, 5:6, :] = jnp.where(taking, 1.0, 0.0) + jnp.zeros((1, BLOCK), F32)
    for rel in range(1, 4):
        for p in range(4):
            wbuf[rel, p, 3, :, :128] = jnp.zeros((WROWS, 128), BF16)
    own_b.wait()
    bbuf[0, zl, :SHARE] = share[...]
    bbuf[0, zl, SHARE:] = jnp.zeros((PADDED - SHARE, share.shape[1]), BF16)
    with scope('barrier'):
        pl.semaphore_wait(barrier, len(peers))

    ids = {}
    sent = []
    sent_by_core = ([], [])
    pieces = {}

    def remote(name, src, dst, device):
        i = ids.setdefault(name, len(ids))
        return pltpu.make_async_remote_copy(
            src_ref=src,
            dst_ref=dst,
            send_sem=ssem.at[i],
            recv_sem=rsem.at[i],
            device_id=device,
            device_id_type=pl.DeviceIdType.MESH,
        )

    def send(name, src, dst, device, into=sent):
        copy = remote(name, src, dst, device)
        copy.start()
        into.append(copy if into is sent else (name, device))

    def got(name, landing, device):
        with scope("got_" + name):
            remote(name, landing, landing, device).wait_recv()

    local_ids = {}

    def local(name, src, dst):
        i = local_ids.setdefault(name, len(local_ids))
        assert i < 20
        copy = pltpu.make_async_copy(src, dst, lsem.at[i])
        copy.start()
        return copy

    oz = 1 - zl
    around = (u, um, up, u2)
    order = (v, vm, vp, v2)

    def b_half(kv, ku, zz):
        return bbuf.at[place_of(kv, ku), zz]

    def b_at(kv, ku):
        return bbuf.at[place_of(kv, ku)]

    kinds = {"full": (128, 640), "lower": (128, 256), "upper": (384, 384)}

    def w_copies(kind, p, q):
        lanes = kinds[kind]
        yield "a", (16, WROWS - 16), lanes, None
        yield "b", (0, 16), lanes, p != 3
        if kind != "upper":
            yield "c", (0, WROWS), (0, 128), q != 3

    def guarded(needed, run):
        if needed is None:
            run()
        else:
            pl.when(needed)(run)

    def w_own(p, q):
        def view(rows, lanes):
            row = pl.multiple_of(c * 368 + p * WROWS - 16 * (p // 3) + rows[0], 16)
            col = pl.multiple_of(q * WCOLS - 128 * (q // 3) + lanes[0], 128)
            return w_ref.at[pl.ds(row, rows[1]), pl.ds(col, lanes[1])]

        return view

    def w_one(rel):
        return lambda rows, lanes: wbuf.at[rel, u, v, pl.ds(*rows), pl.ds(*lanes)]

    def w_at(uu, vv):
        return lambda rows, lanes: wbuf.at[pl.ds(1, 3), uu, vv, pl.ds(*rows), pl.ds(*lanes)]

    w_sent = []

    def w_move(name, src, dst, device, p, q, kind="full"):
        for tag, rows, lanes, needed in w_copies(kind, p, q):
            guarded(
                needed,
                lambda: remote(name + tag, src(rows, lanes), dst(rows, lanes), device).start(),
            )
        w_sent.append((name, src, device, p, q, kind))

    def w_got(name, landing, device, p, q, kind="full"):
        with scope("got_" + name):
            for tag, rows, lanes, needed in w_copies(kind, p, q):

                def run():
                    here = landing(rows, lanes)
                    remote(name + tag, here, here, device).wait_recv()

                guarded(needed, run)

    def w_left(name, src, device, p, q, kind):
        for tag, rows, lanes, needed in w_copies(kind, p, q):

            def run():
                here = src(rows, lanes)
                remote(name + tag, here, here, device).wait_send()

            guarded(needed, run)

    def w_send(uu, tag):
        w_move(f"wv_p{tag}", w_at(uu, v), w_at(uu, v), dev_vp, uu, v)
        w_move(f"wv_m{tag}", w_at(uu, v), w_at(uu, v), dev_vm, uu, v)

    def b_send(ku):
        for name, kv, device in ((f"bv_p{ku}", 1, dev_vp), (f"bv_m{ku}", 2, dev_vm)):
            remote(name, b_at(0, ku), b_at(kv, ku), device).start()
            pieces[name] = device

    def b_got(kv, ku):
        if ku:
            got(f"bv_{'pm'[kv - 1]}{ku}", b_at(kv, ku), dev_vm if kv == 1 else dev_vp)
        else:
            for zz, tag in ((zl, "a"), (oz, "b")):
                device = dev_vm if kv == 1 else dev_vp
                got(f"bv_{'pm'[kv - 1]}0{tag}", b_half(kv, 0, zz), device)

    def far_line(step, core=None):
        def core0():
            for kv, ku in (((1, 0),), ((1, 1),), ((2, 2),), ((2, 3),), ())[step]:
                device = dev_vp if kv == 1 else dev_vm
                send(f"bf{kv}{ku}", b_at(kv, ku), b_at(3, ku), device, sent_by_core[0])
            if step == 4:
                for ku in range(4):
                    got(f"bf{1 if ku < 2 else 2}{ku}", b_at(3, ku), dev_vm if ku < 2 else dev_vp)

        def core1():
            into = sent_by_core[1]
            if step == 0:
                send("bx_p", b_half(1, 0, zl), b_half(3, 0, zl), dev_vp, into)
                send("bx_m", b_half(2, 0, oz), b_half(3, 0, oz), dev_vm, into)
            elif step == 1:
                pass
            elif step == 2:
                got("bx_p", b_half(3, 0, zl), dev_vm)
                got("bx_m", b_half(3, 0, oz), dev_vp)
                send("by_p", b_at(3, 0), b_at(3, 1), dev_up, into)
                send("by_m", b_at(3, 0), b_at(3, 2), dev_um, into)
            elif step == 3:
                got("by_p", b_at(3, 1), dev_um)
                send("byf_p", b_half(3, 1, zl), b_half(3, 3, zl), dev_up, into)
                got("by_m", b_at(3, 2), dev_up)
                send("byf_m", b_half(3, 2, oz), b_half(3, 3, oz), dev_um, into)
            else:
                got("byf_p", b_half(3, 3, zl), dev_um)
                got("byf_m", b_half(3, 3, oz), dev_up)

        if core != 1:
            pl.when(c == 0)(core0)
        if core != 0:
            pl.when(c == 1)(core1)

    send("zl", b_half(0, 0, zl), b_half(0, 0, zl), dev_zl)
    send("bu_p0", b_half(0, 0, zl), b_half(0, 1, zl), dev_up)
    send("bu_m0", b_half(0, 0, zl), b_half(0, 2, zl), dev_um)
    send("meta_far", meta_buf.at[0], meta_buf.at[1], dev_far)
    own_a = []
    for j in range(3):
        own_a.append(local(f"a{j}", a_ref.at[j], a_all.at[2 * j + c]))
        send(f"mate_a{j}", a_ref.at[j], a_all.at[2 * j + c], dev_mate)
    own_a.append(local("a3", a_ref.at[3], own3))
    send("bv_p0a", b_half(0, 0, zl), b_half(1, 0, zl), dev_vp)
    send("bv_m0a", b_half(0, 0, zl), b_half(2, 0, zl), dev_vm)

    got("zl", b_half(0, 0, oz), dev_zl)
    send("bu_p1", b_half(0, 0, oz), b_half(0, 1, oz), dev_up)
    send("bu_m1", b_half(0, 0, oz), b_half(0, 2, oz), dev_um)
    send("bv_p0b", b_half(0, 0, oz), b_half(1, 0, oz), dev_vp)
    send("bv_m0b", b_half(0, 0, oz), b_half(2, 0, oz), dev_vm)
    w_move("wz_m", w_own(u, v), w_one(1), dev_hm, u, v)
    w_move("wz_p", w_own(u, v), w_one(3), dev_hp, u, v)

    got("bu_p0", b_half(0, 1, zl), dev_um)
    send("buf_p", b_half(0, 1, zl), b_half(0, 3, zl), dev_up)
    got("bu_m0", b_half(0, 2, zl), dev_up)
    got("bu_m1", b_half(0, 2, oz), dev_up)
    send("buf_m", b_half(0, 2, oz), b_half(0, 3, oz), dev_um)
    near, far = pl.ds(0, BLOCK // 2), pl.ds(BLOCK // 2, BLOCK // 2)
    send("spare_p", a_ref.at[4, near], relay.at[0], dev_xp)
    send("spare_m", a_ref.at[4, far], relay.at[1], dev_xm)
    got("bu_p1", b_half(0, 1, oz), dev_um)
    b_send(1)
    pl.when(c == 0)(lambda: b_send(2))
    w_got("wz_m", w_one(1), dev_hp, u, v)
    w_move("wzf_m", w_one(1), w_one(2), dev_hm, u, v, "lower")
    w_got("wz_p", w_one(3), dev_hm, u, v)
    w_move("wzf_p", w_one(3), w_one(2), dev_hp, u, v, "upper")
    for j in range(3):
        own_a[j].wait()
        got(f"mate_a{j}", a_all.at[2 * j + 1 - c], dev_mate)
    got("buf_p", b_half(0, 3, zl), dev_um)
    got("buf_m", b_half(0, 3, oz), dev_up)

    def slot_of(r, cc):
        return (h + r + 7 - 2 * cc - zl) % 4

    def half(cc):
        return pl.ds(cc * BLOCK, BLOCK)

    def project(k, j):
        lo, hi = CHUNKS[k]
        rows = (hi - lo) * PIECE
        part[j, lo:hi] = lax.dot_general(
            bbuf[lo:hi].reshape(rows, bbuf.shape[-1]),
            a_all[pl.ds(2 * j, 2)].reshape(2 * BLOCK, bbuf.shape[-1]),
            (((1,), (1,)), ((), ())),
            preferred_element_type=F32,
        ).reshape(hi - lo, PIECE, 2 * BLOCK)

    def span(k):
        return pl.ds(CHUNKS[k][0], CHUNKS[k][1] - CHUNKS[k][0])

    chunks_sent = {}

    def phase(late, j, run):
        pl.when((j == 3) if late else (j != 3))(run)

    def compute(k, late):
        with scope(f"compute{k}_{late}"):
            if late:
                project(k, 3)
            else:

                @pl.loop(0, 3)
                def _(j):
                    project(k, j)

            for name, i, r, cc, send_buf, recv_buf, device in (
                ("hop", 0, 2, 0, hop_s, hop_r, dev_hm),
                ("hop", 1, 2, 1, hop_s, hop_r, dev_hp),
                ("dir", 0, 3, 1, dir_s, dir_r, dev_hm),
                ("dir", 1, 1, 0, dir_s, dir_r, dev_hp),
            ):
                j = slot_of(r, cc)
                copy = remote(
                    f"{name}{k}{i}", send_buf.at[i, span(k)], recv_buf.at[i, span(k)], device
                )
                chunks_sent[f"{name}{k}{i}"] = (f"{name}{k}{i}", k, i, device)

                def run():
                    send_buf[i, span(k)] = part[j, span(k), :, half(cc)].astype(BF16)
                    copy.start()

                phase(late, j, run)

    def combine(k, late, core=None):
        for i, r, cc, source, device in ((0, 3, 0, dev_hp, dev_hm), (1, 1, 1, dev_hm, dev_hp)):
            j = slot_of(r, cc)
            copy = remote(
                f"comb{k}{i}", comb_s.at[i, span(k)], comb_r.at[i, span(k)], device
            )
            chunks_sent[f"comb{k}{i}"] = (f"comb{k}{i}", k, i, device)

            def run():
                got(f"hop{k}{i}", hop_r.at[i, span(k)], source)
                total = part[j, span(k), :, half(cc)] + hop_r[i, span(k)].astype(F32)
                comb_s[i, span(k)] = total.astype(BF16)
                copy.start()

            if core is None:
                phase(late, j, run)
            else:
                pl.when((j != 3) & (c == core))(run)

    def finish(k, late):
        for cc, first, second in ((0, dev_hp, dev_hm), (1, dev_hm, dev_hp)):
            j = slot_of(0, cc)
            mine = pt.at[c, cc, span(k)]
            to_mate = remote(f"pt{k}{cc}", mine, mine, dev_mate)
            if not late:
                sent.append(to_mate)

            def run():
                got(f"dir{k}{1 - cc}", dir_r.at[1 - cc, span(k)], second)
                got(f"comb{k}{cc}", comb_r.at[cc, span(k)], first)
                pt[c, cc, span(k)] = part[j, span(k), :, half(cc)] + (
                    comb_r[cc, span(k)].astype(F32) + dir_r[1 - cc, span(k)].astype(F32)
                )
                to_mate.start()

            phase(late, j, run)

    compute(0, False)

    got("meta_far", meta_buf.at[1], dev_far)
    swap = meta_buf[0, 5:6, :] > 0.5
    for row, far_row in ((0, 4), (8, 12)):
        first = row // 2
        meta_all[c, first : first + 3, :] = meta_buf[0, row : row + 3, :]
        meta_all[c, first + 3 : first + 4, :] = jnp.where(
            swap, meta_buf[1, far_row : far_row + 1, :], meta_buf[0, row + 3 : row + 4, :]
        )
    send("meta_mate", meta_all.at[c], meta_all.at[c], dev_mate)

    b_got(1, 0)
    b_got(2, 0)
    far_line(0)
    compute(1, False)
    got("spare_p", relay.at[0], dev_xm)
    send("spare_pf", relay.at[0], spare.at[near], dev_xp)
    got("spare_m", relay.at[1], dev_xp)
    send("spare_mf", relay.at[1], spare.at[far], dev_xm)
    pl.when(c == 1)(lambda: b_send(2))
    b_send(3)
    combine(0, False, 1)
    b_got(1, 1)
    far_line(1)
    b_got(2, 1)
    compute(2, False)
    combine(0, False, 0)
    far_line(2, 1)

    def fourth():
        b_got(2, 2)
        b_got(1, 2)
        compute(3, False)

    def fifth(core):
        b_got(2, 3)
        if core == 0:
            far_line(3, 0)
        b_got(1, 3)
        compute(4, False)

    @pl.when(c == 0)
    def _():
        b_got(2, 2)
        far_line(2, 0)
        b_got(1, 2)
        compute(3, False)
        combine(1, False, 0)

    got("spare_pf", spare.at[near], dev_xm)
    got("spare_mf", spare.at[far], dev_xp)
    own_a[3].wait()
    a_all[6 + c] = jnp.where(taking, spare[...], own3[...])
    send("mate_a3", a_all.at[6 + c], a_all.at[6 + c], dev_mate)

    @pl.when(c == 0)
    def _():
        fifth(0)
        combine(2, False, 0)

    combine(1, False, 1)
    got("mate_a3", a_all.at[7 - c], dev_mate)
    for k in range(3):
        compute(k, True)

    w_got("wzf_m", w_one(2), dev_hp, u, v, "lower")
    w_got("wzf_p", w_one(2), dev_hm, u, v, "upper")
    w_move("wu_p", w_at(u, v), w_at(u, v), dev_up, u, v)
    w_move("wu_m", w_at(u, v), w_at(u, v), dev_um, u, v)
    own_w = []
    for p in range(4):
        for q in range(4):
            own_w.append(local(f"w{p}{q}", w_own(p, q)((0, WROWS), (0, WCOLS)), wbuf.at[0, p, q]))
    combine(2, False, 1)

    @pl.when(c == 1)
    def _():
        fourth()
        far_line(3, 1)
        fifth(1)

    compute(3, True)
    w_send(u, 0)
    compute(4, True)

    w_got("wu_p", w_at(um, v), dev_um, um, v)
    w_move("wuf_p", w_at(um, v), w_at(um, v), dev_up, um, v, "lower")
    w_send(um, 1)
    w_got("wu_m", w_at(up, v), dev_up, up, v)
    w_move("wuf_m", w_at(up, v), w_at(up, v), dev_um, up, v, "upper")
    w_send(up, 2)
    combine(3, False)
    combine(0, True)
    combine(1, True)
    far_line(4)
    compute(5, False)
    compute(5, True)
    combine(2, True)
    combine(3, True)
    combine(4, False)
    combine(4, True)
    w_got("wuf_p", w_at(u2, v), dev_um, u2, v, "lower")
    w_got("wuf_m", w_at(u2, v), dev_up, u2, v, "upper")
    w_send(u2, 3)
    w_got("wv_p0", w_at(u, vm), dev_vm, u, vm)
    w_move("wvf_p0", w_at(u, vm), w_at(u, vm), dev_vp, u, vm)
    w_got("wv_p1", w_at(um, vm), dev_vm, um, vm)
    w_move("wvf_p1", w_at(um, vm), w_at(um, vm), dev_vp, um, vm)
    combine(5, False)
    w_got("wv_m0", w_at(u, vp), dev_vp, u, vp)
    w_got("wv_m1", w_at(um, vp), dev_vp, um, vp)
    w_got("wv_m2", w_at(up, vp), dev_vp, up, vp)
    w_move("wvf_m2", w_at(up, vp), w_at(up, vp), dev_vm, up, vp)
    combine(5, True)
    w_got("wv_m3", w_at(u2, vp), dev_vp, u2, vp)
    w_move("wvf_m3", w_at(u2, vp), w_at(u2, vp), dev_vm, u2, vp)
    w_got("wv_p2", w_at(up, vm), dev_vm, up, vm)
    w_got("wv_p3", w_at(u2, vm), dev_vm, u2, vm)
    for k in range(6):
        finish(k, False)
        finish(k, True)
    for k in range(6):
        for cc in range(2):
            got(f"pt{k}{cc}", pt.at[1 - c, cc, span(k)], dev_mate)

    def rank(there, here):
        step = (2 * ((there + 4 - here) % 4)) % 5
        return step - step // 4

    with scope("assemble"):
        for src in range(2):
            own = c == src
            u_src, v_src = jnp.where(own, u, v), jnp.where(own, v, u)
            for vv in range(4):
                kv = rank(vv, v_src)
                for uu in range(4):
                    ku = rank(uu, u_src)
                    place = jnp.where(kv == 3, 12 + ku, 3 + 2 * ku + kv)
                    place = jnp.where(kv == 0, ku, place)
                    for zz in range(2):
                        xx, yy = (uu, vv) if src == 0 else (vv, uu)
                        first = SHARE * (xx * 16 + zz * 8 + yy * 2 + src)
                        row = PADDED * zz
                        for cc in range(2):
                            ptd[first : first + SHARE, half(cc)] = pt[
                                src, cc, place, row : row + SHARE, :
                            ]
        high = ptd[...].astype(BF16)
        ptd_h[...] = high
        ptd_l[...] = (ptd[...] - high.astype(F32)).astype(BF16)
        for q in range(3):
            pth[q] = high[q * WCOLS : (q + 1) * WCOLS, :]
        pth[3, :128] = jnp.zeros((128, 2 * BLOCK), BF16)
        pth[3, 128:] = high[3 * WCOLS :, :]

    for copy in own_w:
        copy.wait()

    def screened(rel, q):
        return jnp.dot(
            wbuf[rel, :, q].reshape(4 * WROWS, WCOLS), pth[q], preferred_element_type=F32
        )

    def rows_of(rel):
        return pl.ds(pl.multiple_of(rel * 4 * WROWS, 4 * WROWS), 4 * WROWS)

    with scope("screen"):

        @pl.loop(0, 4)
        def _(rel):
            scr[rows_of(rel), :] = screened(rel, v) + screened(rel, vm) + screened(rel, vp)

    for tag in range(4):
        if tag < 2:
            w_got(f"wvf_p{tag}", w_at(around[tag], v2), dev_vm, around[tag], v2)
        else:
            w_got(f"wvf_m{tag}", w_at(around[tag], v2), dev_vp, around[tag], v2)
    with scope("screen_last"):

        @pl.loop(0, 4)
        def _(rel):
            value = scr[rows_of(rel), :] + screened(rel, v2)
            high = value.astype(BF16)
            scr_h[rows_of(rel), :] = high
            scr_l[rows_of(rel), :] = (value - high.astype(F32)).astype(BF16)

    with scope("bs"):
        for slot in range(2):
            total = jnp.zeros((BLOCK, BLOCK), F32)
            for rel in range(4):
                base = ((h + rel) % 4) * 736 + c * 368
                for skip, first, count in ((0, 0, 288), (304, 288, 80)):
                    left_rows = pl.ds(rel * 4 * WROWS + skip, count)
                    right_rows = pl.ds(pl.multiple_of(base + first, 16), count)
                    for left, right in ((scr_h, ptd_h), (scr_h, ptd_l), (scr_l, ptd_h)):
                        total += lax.dot_general(
                            left[left_rows, half(slot)],
                            right[right_rows, half(slot)],
                            (((0,), (0,)), ((), ())),
                            preferred_element_type=F32,
                        )
            bs_own[slot] = total
    send("bs", bs_own, bs_mate, dev_mate)

    got("meta_mate", meta_all.at[1 - c], dev_mate)
    with scope("places"):
        item = lax.broadcasted_iota(jnp.int32, (NB_SIGMA // 2, BLOCK), 0)
        rows = (item // 64) * 128 + (item // 8) % 2 * 64 + (item // 16) % 4 * 16 + c * 8 + item % 8
        rows = rows.astype(F32)
        columns = lax.broadcasted_iota(jnp.int32, (NB_SIGMA, BLOCK), 0).astype(F32)
        places = []
        for cc in range(2):
            j = slot_of(0, cc)
            index = meta_all[cc, pl.ds(j, 1), :]
            weight = meta_all[cc, pl.ds(4 + j, 1), :]
            places.append(((rows == index).astype(BF16), (columns == index).astype(BF16), weight))
    got("bs", bs_mate, dev_mate)
    with scope("spread"):
        spread = jnp.zeros((NB_SIGMA // 2, NB_SIGMA), F32)
        for slot in range(2):
            to_rows, to_columns, weight = places[slot]
            block = (bs_own[slot] + bs_mate[slot]) * weight
            high = block.astype(BF16)
            low = (block - high.astype(F32)).astype(BF16)
            for term in (high, low):
                wide = lax.dot_general(
                    term, to_columns, (((1,), (1,)), ((), ())), preferred_element_type=F32
                )
                spread += jnp.dot(to_rows, wide.astype(BF16), preferred_element_type=F32)
        plane_s[...] = spread.astype(BF16).reshape(4, 4, 16, NB_SIGMA)
    early = len(sent)
    for (dx, dy), (place, device) in plane.items():
        send(f"plane{dx}{dy}", plane_s.at[place[0], place[1]], plane_r.at[x, y], device)
    for copy in sent[:early]:
        copy.wait_send()
    del sent[:early]
    for item in w_sent:
        w_left(*item)
    for name, device in pieces.items():
        remote(name, b_at(0, 0), b_at(0, 0), device).wait_send()
    for name, k, i, device in chunks_sent.values():
        piece = hop_s.at[i, span(k)]
        remote(name, piece, piece, device).wait_send()
    for core in range(2):

        @pl.when(c == core)
        def _():
            for name, device in sent_by_core[core]:
                whole = core == 0 or name in ("by_p", "by_m")
                piece = b_at(0, 0) if whole else b_half(0, 0, 0)
                remote(name, piece, piece, device).wait_send()

    total = plane_s[x, y].astype(F32)
    for dx, dy in plane:
        source = (x + 4 - dx) % 4, (y + 4 - dy) % 4
        landed = plane_r.at[source[0], source[1]]
        got(f"plane{dx}{dy}", landed, plane[(4 - dx) % 4, (4 - dy) % 4][1])
        total += landed[...].astype(F32)
    for zz in range(2):
        for hh in range(4):
            first = 8 * zz + 2 * hh
            line_s[zz, hh] = total[first : first + 2, :]
    for (dz, dh), (place, device) in line.items():
        send(f"line{dz}{dh}", line_s.at[place[0], place[1]], line_r.at[zl, h], device)
    result = line_s[zl, h]
    for dz, dh in line:
        source = (zl + dz) % 2, (h + 4 - dh) % 4
        landed = line_r.at[source[0], source[1]]
        got(f"line{dz}{dh}", landed, line[dz, (4 - dh) % 4][1])
        result += landed[...]
    out_ref[...] = result
    for copy in sent:
        copy.wait_send()
    assert len(ids) == N_COPIES


def per_device(pair_density, eigvecs, screening, occupation, window_start, window_len, slot_band):
    block, plane_rows = pair_density.shape[1:]
    width = screening.shape[1]
    vmem = pl.BlockSpec(memory_space=pltpu.VMEM)
    hbm = pl.BlockSpec(memory_space=pltpu.HBM)
    scratch = [
        pltpu.VMEM((8, block, plane_rows), BF16),
        pltpu.VMEM((block, plane_rows), BF16),
        pltpu.VMEM((2, block // 2, plane_rows), BF16),
        pltpu.VMEM((block, plane_rows), BF16),
        pltpu.VMEM((SHARE, plane_rows), BF16),
        pltpu.VMEM((16, 2, PADDED, plane_rows), BF16),
        pltpu.VMEM((4, 4, 4, WROWS, WCOLS), BF16),
        pltpu.VMEM((4, 16, PIECE, 2 * block), F32),
    ]
    scratch += [pltpu.VMEM((2, 16, PIECE, block), BF16)] * 6
    scratch += [
        pltpu.VMEM((2, 2, 16, PIECE, block), F32),
        pltpu.VMEM((width, 2 * block), F32),
        pltpu.VMEM((4, WCOLS, 2 * block), BF16),
        pltpu.VMEM((width, 2 * block), BF16),
        pltpu.VMEM((width, 2 * block), BF16),
        pltpu.VMEM((16 * WROWS, 2 * block), F32),
        pltpu.VMEM((16 * WROWS, 2 * block), BF16),
        pltpu.VMEM((16 * WROWS, 2 * block), BF16),
        pltpu.VMEM((2, 16, block), F32),
        pltpu.VMEM((2, 8, block), F32),
        pltpu.VMEM((2, block, block), F32),
        pltpu.VMEM((2, block, block), F32),
        pltpu.VMEM((4, 4, 16, NB_SIGMA), BF16),
        pltpu.VMEM((4, 4, 16, NB_SIGMA), BF16),
        pltpu.VMEM((2, 4, 2, NB_SIGMA), F32),
        pltpu.VMEM((2, 4, 2, NB_SIGMA), F32),
        pltpu.SemaphoreType.DMA((N_COPIES,)),
        pltpu.SemaphoreType.DMA((N_COPIES,)),
        pltpu.SemaphoreType.DMA((21,)),
    ]
    smem = pl.BlockSpec(memory_space=pltpu.SMEM)
    return pl.pallas_call(
        main_kernel,
        out_shape=jax.ShapeDtypeStruct((2, NB_SIGMA), F32),
        in_specs=[smem, smem, smem, vmem, hbm, hbm, hbm],
        out_specs=vmem,
        scratch_shapes=scratch,
        compiler_params=pltpu.CompilerParams(
            collective_id=0, has_side_effects=True, vmem_limit_bytes=60 * 1024 * 1024
        ),
        name="cohsex",
    )(
        window_start,
        window_len,
        slot_band,
        occupation.reshape(1, -1),
        pair_density,
        eigvecs,
        screening,
    )


def solution(mesh):
    return jax.shard_map(
        per_device,
        mesh=mesh,
        in_specs=(
            P("band", None, "pw"),
            P("band", "pw"),
            P("pw", None),
            P(),
            P("band"),
            P("band"),
            P("band"),
        ),
        out_specs=P(("band", "pw"), None),
        check_vma=False,
    )
```

```python
import jax
import jax.numpy as jnp
from jax import lax
from jax.experimental import pallas as pl
from jax.experimental.pallas import tpu as pltpu
from jax.sharding import PartitionSpec as P

NB_SIGMA = 512
BLOCK = 128
F32 = jnp.float32
BF16 = jnp.bfloat16
HIGHEST = lax.Precision.HIGHEST
SHARE, PADDED = 46, 48
PIECE = 2 * PADDED
CHUNKS = ((0, 4), (4, 6), (6, 8), (8, 10), (10, 12), (12, 16))


def place_of(kv, ku):
    if kv == 0:
        return ku
    return 12 + ku if kv == 3 else 3 + 2 * ku + kv


WROWS, WCOLS = 96, 768
N_COPIES = 166
scope = jax.named_scope


def main_kernel(
    start_ref,
    len_ref,
    slot_ref,
    occ_ref,
    a_ref,
    eig_ref,
    w_ref,
    out_ref,
    a_all,
    spare,
    relay,
    own3,
    share,
    bbuf,
    wbuf,
    part,
    hop_s,
    hop_r,
    dir_s,
    dir_r,
    comb_s,
    comb_r,
    pt,
    ptd,
    pth,
    ptd_h,
    ptd_l,
    scr,
    scr_h,
    scr_l,
    meta_buf,
    meta_all,
    bs_own,
    bs_mate,
    plane_s,
    plane_r,
    line_s,
    line_r,
    ssem,
    rsem,
    lsem,
):
    band = lax.axis_index("band")
    h = lax.axis_index("pw")
    x = band // 16
    zl = (band // 8) % 2
    y = (band // 2) % 4
    c = band % 2
    u = x * (1 - c) + y * c
    v = y * (1 - c) + x * c
    su = 16 - 14 * c
    sv = 2 + 14 * c
    hp, hm, h2 = (h + 1) % 4, (h + 3) % 4, (h + 2) % 4
    up, um, u2 = (u + 1) % 4, (u + 3) % 4, (u + 2) % 4
    vp, vm, v2 = (v + 1) % 4, (v + 3) % 4, (v + 2) % 4

    def at_uv(uu, vv):
        return (uu * su + vv * sv + zl * 8 + c, h)

    dev_up, dev_um = at_uv(up, v), at_uv(um, v)
    dev_vp, dev_vm = at_uv(u, vp), at_uv(u, vm)
    dev_hp, dev_hm = (band, hp), (band, hm)
    dev_zl = (x * 16 + (1 - zl) * 8 + y * 2 + c, h)
    dev_mate = (x * 16 + zl * 8 + y * 2 + 1 - c, h)
    dev_far = (((x + 2) % 4) * 16 + zl * 8 + y * 2 + c, h)

    barrier = pltpu.get_barrier_semaphore()
    plane = {}
    for dx in range(4):
        for dy in range(4):
            if dx or dy:
                place = ((x + dx) % 4, (y + dy) % 4)
                plane[dx, dy] = place, (place[0] * 16 + zl * 8 + place[1] * 2 + c, h)
    line = {}
    for dz in range(2):
        for dh in range(4):
            if dz or dh:
                place = ((zl + dz) % 2, (h + dh) % 4)
                line[dz, dh] = place, (x * 16 + place[0] * 8 + y * 2 + c, place[1])
    dev_xp, dev_xm = plane[1, 0][1], plane[3, 0][1]
    peers = [dev_mate, dev_up, dev_um, dev_vp, dev_vm, dev_hp, dev_hm, dev_zl, dev_far]
    for peer in peers:
        pl.semaphore_signal(barrier, inc=1, device_id=peer, device_id_type=pl.DeviceIdType.MESH)

    own_b = pltpu.make_async_copy(eig_ref, share, lsem.at[5])
    own_b.start()
    lane = lax.broadcasted_iota(jnp.int32, (1, BLOCK), 1)
    for j in range(5):
        kept = (lane < len_ref[j]) & (slot_ref[j] >= 0)
        meta_buf[0, j : j + 1, :] = jnp.where(kept, start_ref[j] + lane, -1).astype(F32)
        value = jnp.sum(jnp.where(lane == slot_ref[j], occ_ref[...], 0.0), axis=1, keepdims=True)
        meta_buf[0, 8 + j : 9 + j, :] = jnp.broadcast_to(0.5 - value, (1, BLOCK))
    taking = slot_ref[3] < 0
    meta_buf[0, 5:6, :] = jnp.where(taking, 1.0, 0.0) + jnp.zeros((1, BLOCK), F32)
    for rel in range(1, 4):
        for p in range(4):
            wbuf[rel, p, 3, :, :128] = jnp.zeros((WROWS, 128), BF16)
    own_b.wait()
    bbuf[0, zl, :SHARE] = share[...]
    bbuf[0, zl, SHARE:] = jnp.zeros((PADDED - SHARE, share.shape[1]), BF16)
    with scope('barrier'):
        pl.semaphore_wait(barrier, len(peers))

    ids = {}
    sent = []
    sent_by_core = ([], [])
    pieces = {}

    def remote(name, src, dst, device):
        i = ids.setdefault(name, len(ids))
        return pltpu.make_async_remote_copy(
            src_ref=src,
            dst_ref=dst,
            send_sem=ssem.at[i],
            recv_sem=rsem.at[i],
            device_id=device,
            device_id_type=pl.DeviceIdType.MESH,
        )

    def send(name, src, dst, device, into=sent):
        copy = remote(name, src, dst, device)
        copy.start()
        into.append(copy if into is sent else (name, device))

    def got(name, landing, device):
        with scope("got_" + name):
            remote(name, landing, landing, device).wait_recv()

    local_ids = {}

    def local(name, src, dst):
        i = local_ids.setdefault(name, len(local_ids))
        assert i < 4
        copy = pltpu.make_async_copy(src, dst, lsem.at[i])
        copy.start()
        return copy

    oz = 1 - zl
    around = (u, um, up, u2)
    order = (v, vm, vp, v2)

    def b_half(kv, ku, zz):
        return bbuf.at[place_of(kv, ku), zz]

    def b_at(kv, ku):
        return bbuf.at[place_of(kv, ku)]

    kinds = {"full": (128, 640), "lower": (128, 256), "upper": (384, 384)}

    def w_copies(kind, p, q):
        lanes = kinds[kind]
        yield "a", (16, WROWS - 16), lanes, None
        yield "b", (0, 16), lanes, p != 3
        if kind != "upper":
            yield "c", (0, WROWS), (0, 128), q != 3

    def guarded(needed, run):
        if needed is None:
            run()
        else:
            pl.when(needed)(run)

    def w_own(p, q):
        def view(rows, lanes):
            row = pl.multiple_of(c * 368 + p * WROWS - 16 * (p // 3) + rows[0], 16)
            col = pl.multiple_of(q * WCOLS - 128 * (q // 3) + lanes[0], 128)
            return w_ref.at[pl.ds(row, rows[1]), pl.ds(col, lanes[1])]

        return view

    def w_one(rel):
        return lambda rows, lanes: wbuf.at[rel, u, v, pl.ds(*rows), pl.ds(*lanes)]

    def w_at(uu, vv):
        return lambda rows, lanes: wbuf.at[pl.ds(1, 3), uu, vv, pl.ds(*rows), pl.ds(*lanes)]

    w_sent = []

    def w_move(name, src, dst, device, p, q, kind="full"):
        for tag, rows, lanes, needed in w_copies(kind, p, q):
            guarded(
                needed,
                lambda: remote(name + tag, src(rows, lanes), dst(rows, lanes), device).start(),
            )
        w_sent.append((name, src, device, p, q, kind))

    def w_got(name, landing, device, p, q, kind="full"):
        with scope("got_" + name):
            for tag, rows, lanes, needed in w_copies(kind, p, q):

                def run():
                    here = landing(rows, lanes)
                    remote(name + tag, here, here, device).wait_recv()

                guarded(needed, run)

    def w_left(name, src, device, p, q, kind):
        for tag, rows, lanes, needed in w_copies(kind, p, q):

            def run():
                here = src(rows, lanes)
                remote(name + tag, here, here, device).wait_send()

            guarded(needed, run)

    def w_send(uu, tag):
        w_move(f"wv_p{tag}", w_at(uu, v), w_at(uu, v), dev_vp, uu, v)
        w_move(f"wv_m{tag}", w_at(uu, v), w_at(uu, v), dev_vm, uu, v)

    def b_send(ku):
        for name, kv, device in ((f"bv_p{ku}", 1, dev_vp), (f"bv_m{ku}", 2, dev_vm)):
            remote(name, b_at(0, ku), b_at(kv, ku), device).start()
            pieces[name] = device

    def b_got(kv, ku):
        if ku:
            got(f"bv_{'pm'[kv - 1]}{ku}", b_at(kv, ku), dev_vm if kv == 1 else dev_vp)
        else:
            for zz, tag in ((zl, "a"), (oz, "b")):
                device = dev_vm if kv == 1 else dev_vp
                got(f"bv_{'pm'[kv - 1]}0{tag}", b_half(kv, 0, zz), device)

    def far_line(step, core=None):
        def core0():
            for kv, ku in (((1, 0),), ((1, 1),), ((2, 2),), ((2, 3),), ())[step]:
                device = dev_vp if kv == 1 else dev_vm
                send(f"bf{kv}{ku}", b_at(kv, ku), b_at(3, ku), device, sent_by_core[0])
            if step == 4:
                for ku in range(4):
                    got(f"bf{1 if ku < 2 else 2}{ku}", b_at(3, ku), dev_vm if ku < 2 else dev_vp)

        def core1():
            into = sent_by_core[1]
            if step == 0:
                send("bx_p", b_half(1, 0, zl), b_half(3, 0, zl), dev_vp, into)
                send("bx_m", b_half(2, 0, oz), b_half(3, 0, oz), dev_vm, into)
            elif step == 1:
                pass
            elif step == 2:
                got("bx_p", b_half(3, 0, zl), dev_vm)
                got("bx_m", b_half(3, 0, oz), dev_vp)
                send("by_p", b_at(3, 0), b_at(3, 1), dev_up, into)
                send("by_m", b_at(3, 0), b_at(3, 2), dev_um, into)
            elif step == 3:
                got("by_p", b_at(3, 1), dev_um)
                send("byf_p", b_half(3, 1, zl), b_half(3, 3, zl), dev_up, into)
                got("by_m", b_at(3, 2), dev_up)
                send("byf_m", b_half(3, 2, oz), b_half(3, 3, oz), dev_um, into)
            else:
                got("byf_p", b_half(3, 3, zl), dev_um)
                got("byf_m", b_half(3, 3, oz), dev_up)

        if core != 1:
            pl.when(c == 0)(core0)
        if core != 0:
            pl.when(c == 1)(core1)

    send("zl", b_half(0, 0, zl), b_half(0, 0, zl), dev_zl)
    send("bu_p0", b_half(0, 0, zl), b_half(0, 1, zl), dev_up)
    send("bu_m0", b_half(0, 0, zl), b_half(0, 2, zl), dev_um)
    send("meta_far", meta_buf.at[0], meta_buf.at[1], dev_far)
    own_a = []
    for j in range(3):
        own_a.append(local(f"a{j}", a_ref.at[j], a_all.at[2 * j + c]))
        send(f"mate_a{j}", a_ref.at[j], a_all.at[2 * j + c], dev_mate)
    own_a.append(local("a3", a_ref.at[3], own3))
    send("bv_p0a", b_half(0, 0, zl), b_half(1, 0, zl), dev_vp)
    send("bv_m0a", b_half(0, 0, zl), b_half(2, 0, zl), dev_vm)

    got("zl", b_half(0, 0, oz), dev_zl)
    send("bu_p1", b_half(0, 0, oz), b_half(0, 1, oz), dev_up)
    send("bu_m1", b_half(0, 0, oz), b_half(0, 2, oz), dev_um)
    send("bv_p0b", b_half(0, 0, oz), b_half(1, 0, oz), dev_vp)
    send("bv_m0b", b_half(0, 0, oz), b_half(2, 0, oz), dev_vm)
    w_move("wz_m", w_own(u, v), w_one(1), dev_hm, u, v)
    w_move("wz_p", w_own(u, v), w_one(3), dev_hp, u, v)

    got("bu_p0", b_half(0, 1, zl), dev_um)
    send("buf_p", b_half(0, 1, zl), b_half(0, 3, zl), dev_up)
    got("bu_m0", b_half(0, 2, zl), dev_up)
    got("bu_m1", b_half(0, 2, oz), dev_up)
    send("buf_m", b_half(0, 2, oz), b_half(0, 3, oz), dev_um)
    near, far = pl.ds(0, BLOCK // 2), pl.ds(BLOCK // 2, BLOCK // 2)
    send("spare_p", a_ref.at[4, near], relay.at[0], dev_xp)
    send("spare_m", a_ref.at[4, far], relay.at[1], dev_xm)
    got("bu_p1", b_half(0, 1, oz), dev_um)
    b_send(1)
    pl.when(c == 0)(lambda: b_send(2))
    w_got("wz_m", w_one(1), dev_hp, u, v)
    w_move("wzf_m", w_one(1), w_one(2), dev_hm, u, v, "lower")
    w_got("wz_p", w_one(3), dev_hm, u, v)
    w_move("wzf_p", w_one(3), w_one(2), dev_hp, u, v, "upper")
    for j in range(3):
        own_a[j].wait()
        got(f"mate_a{j}", a_all.at[2 * j + 1 - c], dev_mate)
    got("buf_p", b_half(0, 3, zl), dev_um)
    got("buf_m", b_half(0, 3, oz), dev_up)

    def slot_of(r, cc):
        return (h + r + 7 - 2 * cc - zl) % 4

    def half(cc):
        return pl.ds(cc * BLOCK, BLOCK)

    def project(k, j):
        lo, hi = CHUNKS[k]
        rows = (hi - lo) * PIECE
        part[j, lo:hi] = lax.dot_general(
            bbuf[lo:hi].reshape(rows, bbuf.shape[-1]),
            a_all[pl.ds(2 * j, 2)].reshape(2 * BLOCK, bbuf.shape[-1]),
            (((1,), (1,)), ((), ())),
            preferred_element_type=F32,
        ).reshape(hi - lo, PIECE, 2 * BLOCK)

    def span(k):
        return pl.ds(CHUNKS[k][0], CHUNKS[k][1] - CHUNKS[k][0])

    chunks_sent = {}

    def phase(late, j, run):
        pl.when((j == 3) if late else (j != 3))(run)

    def compute(k, late):
        with scope(f"compute{k}_{late}"):
            if late:
                project(k, 3)
            else:

                @pl.loop(0, 3)
                def _(j):
                    project(k, j)

            for name, i, r, cc, send_buf, recv_buf, device in (
                ("hop", 0, 2, 0, hop_s, hop_r, dev_hm),
                ("hop", 1, 2, 1, hop_s, hop_r, dev_hp),
                ("dir", 0, 3, 1, dir_s, dir_r, dev_hm),
                ("dir", 1, 1, 0, dir_s, dir_r, dev_hp),
            ):
                j = slot_of(r, cc)
                copy = remote(
                    f"{name}{k}{i}", send_buf.at[i, span(k)], recv_buf.at[i, span(k)], device
                )
                chunks_sent[f"{name}{k}{i}"] = (f"{name}{k}{i}", k, i, device)

                def run():
                    send_buf[i, span(k)] = part[j, span(k), :, half(cc)].astype(BF16)
                    copy.start()

                phase(late, j, run)

    def combine(k, late, core=None):
        for i, r, cc, source, device in ((0, 3, 0, dev_hp, dev_hm), (1, 1, 1, dev_hm, dev_hp)):
            j = slot_of(r, cc)
            copy = remote(
                f"comb{k}{i}", comb_s.at[i, span(k)], comb_r.at[i, span(k)], device
            )
            chunks_sent[f"comb{k}{i}"] = (f"comb{k}{i}", k, i, device)

            def run():
                got(f"hop{k}{i}", hop_r.at[i, span(k)], source)
                total = part[j, span(k), :, half(cc)] + hop_r[i, span(k)].astype(F32)
                comb_s[i, span(k)] = total.astype(BF16)
                copy.start()

            if core is None:
                phase(late, j, run)
            else:
                pl.when((j != 3) & (c == core))(run)

    def finish(k, late):
        for cc, first, second in ((0, dev_hp, dev_hm), (1, dev_hm, dev_hp)):
            j = slot_of(0, cc)
            mine = pt.at[c, cc, span(k)]
            to_mate = remote(f"pt{k}{cc}", mine, mine, dev_mate)
            if not late:
                sent.append(to_mate)

            def run():
                got(f"dir{k}{1 - cc}", dir_r.at[1 - cc, span(k)], second)
                got(f"comb{k}{cc}", comb_r.at[cc, span(k)], first)
                pt[c, cc, span(k)] = part[j, span(k), :, half(cc)] + (
                    comb_r[cc, span(k)].astype(F32) + dir_r[1 - cc, span(k)].astype(F32)
                )
                to_mate.start()

            phase(late, j, run)

    compute(0, False)

    got("meta_far", meta_buf.at[1], dev_far)
    swap = meta_buf[0, 5:6, :] > 0.5
    for row, far_row in ((0, 4), (8, 12)):
        first = row // 2
        meta_all[c, first : first + 3, :] = meta_buf[0, row : row + 3, :]
        meta_all[c, first + 3 : first + 4, :] = jnp.where(
            swap, meta_buf[1, far_row : far_row + 1, :], meta_buf[0, row + 3 : row + 4, :]
        )
    send("meta_mate", meta_all.at[c], meta_all.at[c], dev_mate)

    b_got(1, 0)
    b_got(2, 0)
    far_line(0)
    compute(1, False)
    got("spare_p", relay.at[0], dev_xm)
    send("spare_pf", relay.at[0], spare.at[near], dev_xp)
    got("spare_m", relay.at[1], dev_xp)
    send("spare_mf", relay.at[1], spare.at[far], dev_xm)
    pl.when(c == 1)(lambda: b_send(2))
    b_send(3)
    combine(0, False, 1)
    b_got(1, 1)
    far_line(1)
    b_got(2, 1)
    compute(2, False)
    combine(0, False, 0)
    far_line(2, 1)

    def fourth():
        b_got(2, 2)
        b_got(1, 2)
        compute(3, False)

    def fifth(core):
        b_got(2, 3)
        if core == 0:
            far_line(3, 0)
        b_got(1, 3)
        compute(4, False)

    @pl.when(c == 0)
    def _():
        b_got(2, 2)
        far_line(2, 0)
        b_got(1, 2)
        compute(3, False)
        combine(1, False, 0)

    got("spare_pf", spare.at[near], dev_xm)
    got("spare_mf", spare.at[far], dev_xp)
    own_a[3].wait()
    a_all[6 + c] = jnp.where(taking, spare[...], own3[...])
    send("mate_a3", a_all.at[6 + c], a_all.at[6 + c], dev_mate)

    @pl.when(c == 0)
    def _():
        fifth(0)
        combine(2, False, 0)

    combine(1, False, 1)
    got("mate_a3", a_all.at[7 - c], dev_mate)
    for k in range(3):
        compute(k, True)

    w_got("wzf_m", w_one(2), dev_hp, u, v, "lower")
    w_got("wzf_p", w_one(2), dev_hm, u, v, "upper")
    w_move("wu_p", w_at(u, v), w_at(u, v), dev_up, u, v)
    w_move("wu_m", w_at(u, v), w_at(u, v), dev_um, u, v)
    for p in range(4):
        for q in range(4):
            pltpu.make_async_copy(
                w_own(p, q)((0, WROWS), (0, WCOLS)), wbuf.at[0, p, q], lsem.at[4]
            ).start()
    combine(2, False, 1)

    @pl.when(c == 1)
    def _():
        fourth()
        far_line(3, 1)
        fifth(1)

    compute(3, True)
    w_send(u, 0)
    compute(4, True)

    w_got("wu_p", w_at(um, v), dev_um, um, v)
    w_move("wuf_p", w_at(um, v), w_at(um, v), dev_up, um, v, "lower")
    w_send(um, 1)
    w_got("wu_m", w_at(up, v), dev_up, up, v)
    w_move("wuf_m", w_at(up, v), w_at(up, v), dev_um, up, v, "upper")
    w_send(up, 2)
    combine(3, False)
    combine(0, True)
    combine(1, True)
    far_line(4)
    compute(5, False)
    compute(5, True)
    combine(2, True)
    combine(3, True)
    combine(4, False)
    combine(4, True)
    w_got("wuf_p", w_at(u2, v), dev_um, u2, v, "lower")
    w_got("wuf_m", w_at(u2, v), dev_up, u2, v, "upper")
    w_send(u2, 3)
    w_got("wv_p0", w_at(u, vm), dev_vm, u, vm)
    w_move("wvf_p0", w_at(u, vm), w_at(u, vm), dev_vp, u, vm)
    w_got("wv_p1", w_at(um, vm), dev_vm, um, vm)
    w_move("wvf_p1", w_at(um, vm), w_at(um, vm), dev_vp, um, vm)
    combine(5, False)
    w_got("wv_m0", w_at(u, vp), dev_vp, u, vp)
    w_got("wv_m1", w_at(um, vp), dev_vp, um, vp)
    w_got("wv_m2", w_at(up, vp), dev_vp, up, vp)
    w_move("wvf_m2", w_at(up, vp), w_at(up, vp), dev_vm, up, vp)
    combine(5, True)
    w_got("wv_m3", w_at(u2, vp), dev_vp, u2, vp)
    w_move("wvf_m3", w_at(u2, vp), w_at(u2, vp), dev_vm, u2, vp)
    w_got("wv_p2", w_at(up, vm), dev_vm, up, vm)
    w_got("wv_p3", w_at(u2, vm), dev_vm, u2, vm)
    for k in range(6):
        finish(k, False)
        finish(k, True)
    for k in range(6):
        for cc in range(2):
            got(f"pt{k}{cc}", pt.at[1 - c, cc, span(k)], dev_mate)

    def rank(there, here):
        step = (2 * ((there + 4 - here) % 4)) % 5
        return step - step // 4

    with scope("assemble"):
        for src in range(2):
            own = c == src
            u_src, v_src = jnp.where(own, u, v), jnp.where(own, v, u)
            for vv in range(4):
                kv = rank(vv, v_src)
                for uu in range(4):
                    ku = rank(uu, u_src)
                    place = jnp.where(kv == 3, 12 + ku, 3 + 2 * ku + kv)
                    place = jnp.where(kv == 0, ku, place)
                    for zz in range(2):
                        xx, yy = (uu, vv) if src == 0 else (vv, uu)
                        first = SHARE * (xx * 16 + zz * 8 + yy * 2 + src)
                        row = PADDED * zz
                        for cc in range(2):
                            ptd[first : first + SHARE, half(cc)] = pt[
                                src, cc, place, row : row + SHARE, :
                            ]
        high = ptd[...].astype(BF16)
        ptd_h[...] = high
        ptd_l[...] = (ptd[...] - high.astype(F32)).astype(BF16)
        for q in range(3):
            pth[q] = high[q * WCOLS : (q + 1) * WCOLS, :]
        pth[3, :128] = jnp.zeros((128, 2 * BLOCK), BF16)
        pth[3, 128:] = high[3 * WCOLS :, :]

    pltpu.make_async_copy(wbuf.at[0], wbuf.at[0], lsem.at[4]).wait()

    def screened(rel, q):
        return jnp.dot(
            wbuf[rel, :, q].reshape(4 * WROWS, WCOLS), pth[q], preferred_element_type=F32
        )

    def rows_of(rel):
        return pl.ds(pl.multiple_of(rel * 4 * WROWS, 4 * WROWS), 4 * WROWS)

    with scope("screen"):

        @pl.loop(0, 4)
        def _(rel):
            scr[rows_of(rel), :] = screened(rel, v) + screened(rel, vm) + screened(rel, vp)

    for tag in range(4):
        if tag < 2:
            w_got(f"wvf_p{tag}", w_at(around[tag], v2), dev_vm, around[tag], v2)
        else:
            w_got(f"wvf_m{tag}", w_at(around[tag], v2), dev_vp, around[tag], v2)
    with scope("screen_last"):

        @pl.loop(0, 4)
        def _(rel):
            value = scr[rows_of(rel), :] + screened(rel, v2)
            high = value.astype(BF16)
            scr_h[rows_of(rel), :] = high
            scr_l[rows_of(rel), :] = (value - high.astype(F32)).astype(BF16)

    with scope("bs"):
        for slot in range(2):
            total = jnp.zeros((BLOCK, BLOCK), F32)
            for rel in range(4):
                base = ((h + rel) % 4) * 736 + c * 368
                for skip, first, count in ((0, 0, 288), (304, 288, 80)):
                    left_rows = pl.ds(rel * 4 * WROWS + skip, count)
                    right_rows = pl.ds(pl.multiple_of(base + first, 16), count)
                    for left, right in ((scr_h, ptd_h), (scr_h, ptd_l), (scr_l, ptd_h)):
                        total += lax.dot_general(
                            left[left_rows, half(slot)],
                            right[right_rows, half(slot)],
                            (((0,), (0,)), ((), ())),
                            preferred_element_type=F32,
                        )
            bs_own[slot] = total
    send("bs", bs_own, bs_mate, dev_mate)

    got("meta_mate", meta_all.at[1 - c], dev_mate)
    with scope("places"):
        item = lax.broadcasted_iota(jnp.int32, (NB_SIGMA // 2, BLOCK), 0)
        rows = (item // 64) * 128 + (item // 8) % 2 * 64 + (item // 16) % 4 * 16 + c * 8 + item % 8
        rows = rows.astype(F32)
        columns = lax.broadcasted_iota(jnp.int32, (NB_SIGMA, BLOCK), 0).astype(F32)
        places = []
        for cc in range(2):
            j = slot_of(0, cc)
            index = meta_all[cc, pl.ds(j, 1), :]
            weight = meta_all[cc, pl.ds(4 + j, 1), :]
            places.append(((rows == index).astype(BF16), (columns == index).astype(BF16), weight))
    got("bs", bs_mate, dev_mate)
    with scope("spread"):
        spread = jnp.zeros((NB_SIGMA // 2, NB_SIGMA), F32)
        for slot in range(2):
            to_rows, to_columns, weight = places[slot]
            block = (bs_own[slot] + bs_mate[slot]) * weight
            high = block.astype(BF16)
            low = (block - high.astype(F32)).astype(BF16)
            for term in (high, low):
                wide = lax.dot_general(
                    term, to_columns, (((1,), (1,)), ((), ())), preferred_element_type=F32
                )
                spread += jnp.dot(to_rows, wide.astype(BF16), preferred_element_type=F32)
        plane_s[...] = spread.astype(BF16).reshape(4, 4, 16, NB_SIGMA)
    early = len(sent)
    for (dx, dy), (place, device) in plane.items():
        send(f"plane{dx}{dy}", plane_s.at[place[0], place[1]], plane_r.at[x, y], device)
    for copy in sent[:early]:
        copy.wait_send()
    del sent[:early]
    for item in w_sent:
        w_left(*item)
    for name, device in pieces.items():
        remote(name, b_at(0, 0), b_at(0, 0), device).wait_send()
    for name, k, i, device in chunks_sent.values():
        piece = hop_s.at[i, span(k)]
        remote(name, piece, piece, device).wait_send()
    for core in range(2):

        @pl.when(c == core)
        def _():
            for name, device in sent_by_core[core]:
                whole = core == 0 or name in ("by_p", "by_m")
                piece = b_at(0, 0) if whole else b_half(0, 0, 0)
                remote(name, piece, piece, device).wait_send()

    total = plane_s[x, y].astype(F32)
    for dx, dy in plane:
        source = (x + 4 - dx) % 4, (y + 4 - dy) % 4
        landed = plane_r.at[source[0], source[1]]
        got(f"plane{dx}{dy}", landed, plane[(4 - dx) % 4, (4 - dy) % 4][1])
        total += landed[...].astype(F32)
    for zz in range(2):
        for hh in range(4):
            first = 8 * zz + 2 * hh
            line_s[zz, hh] = total[first : first + 2, :]
    for (dz, dh), (place, device) in line.items():
        send(f"line{dz}{dh}", line_s.at[place[0], place[1]], line_r.at[zl, h], device)
    result = line_s[zl, h]
    for dz, dh in line:
        source = (zl + dz) % 2, (h + 4 - dh) % 4
        landed = line_r.at[source[0], source[1]]
        got(f"line{dz}{dh}", landed, line[dz, (4 - dh) % 4][1])
        result += landed[...]
    out_ref[...] = result
    for copy in sent:
        copy.wait_send()
    assert len(ids) == N_COPIES


def per_device(pair_density, eigvecs, screening, occupation, window_start, window_len, slot_band):
    block, plane_rows = pair_density.shape[1:]
    width = screening.shape[1]
    vmem = pl.BlockSpec(memory_space=pltpu.VMEM)
    hbm = pl.BlockSpec(memory_space=pltpu.HBM)
    scratch = [
        pltpu.VMEM((8, block, plane_rows), BF16),
        pltpu.VMEM((block, plane_rows), BF16),
        pltpu.VMEM((2, block // 2, plane_rows), BF16),
        pltpu.VMEM((block, plane_rows), BF16),
        pltpu.VMEM((SHARE, plane_rows), BF16),
        pltpu.VMEM((16, 2, PADDED, plane_rows), BF16),
        pltpu.VMEM((4, 4, 4, WROWS, WCOLS), BF16),
        pltpu.VMEM((4, 16, PIECE, 2 * block), F32),
    ]
    scratch += [pltpu.VMEM((2, 16, PIECE, block), BF16)] * 6
    scratch += [
        pltpu.VMEM((2, 2, 16, PIECE, block), F32),
        pltpu.VMEM((width, 2 * block), F32),
        pltpu.VMEM((4, WCOLS, 2 * block), BF16),
        pltpu.VMEM((width, 2 * block), BF16),
        pltpu.VMEM((width, 2 * block), BF16),
        pltpu.VMEM((16 * WROWS, 2 * block), F32),
        pltpu.VMEM((16 * WROWS, 2 * block), BF16),
        pltpu.VMEM((16 * WROWS, 2 * block), BF16),
        pltpu.VMEM((2, 16, block), F32),
        pltpu.VMEM((2, 8, block), F32),
        pltpu.VMEM((2, block, block), F32),
        pltpu.VMEM((2, block, block), F32),
        pltpu.VMEM((4, 4, 16, NB_SIGMA), BF16),
        pltpu.VMEM((4, 4, 16, NB_SIGMA), BF16),
        pltpu.VMEM((2, 4, 2, NB_SIGMA), F32),
        pltpu.VMEM((2, 4, 2, NB_SIGMA), F32),
        pltpu.SemaphoreType.DMA((N_COPIES,)),
        pltpu.SemaphoreType.DMA((N_COPIES,)),
        pltpu.SemaphoreType.DMA((6,)),
    ]
    smem = pl.BlockSpec(memory_space=pltpu.SMEM)
    return pl.pallas_call(
        main_kernel,
        out_shape=jax.ShapeDtypeStruct((2, NB_SIGMA), F32),
        in_specs=[smem, smem, smem, vmem, hbm, hbm, hbm],
        out_specs=vmem,
        scratch_shapes=scratch,
        compiler_params=pltpu.CompilerParams(
            collective_id=0, has_side_effects=True, vmem_limit_bytes=60 * 1024 * 1024
        ),
        name="cohsex",
    )(
        window_start,
        window_len,
        slot_band,
        occupation.reshape(1, -1),
        pair_density,
        eigvecs,
        screening,
    )


def solution(mesh):
    return jax.shard_map(
        per_device,
        mesh=mesh,
        in_specs=(
            P("band", None, "pw"),
            P("band", "pw"),
            P("pw", None),
            P(),
            P("band"),
            P("band"),
            P("band"),
        ),
        out_specs=P(("band", "pw"), None),
        check_vma=False,
    )
```
